32 devices in a mesh: patch: 8 (over z, y), sub: 4 (over x, core).
Axes of the slice: x: 2, y: 2, z: 4, core: 2. Of those that a mesh axis runs over, the one named last changes fastest.
Arguments:
- heat: float32 [262144], P(('patch', 'sub')), may hold values from -6 to 6
- basis: bfloat16 [9, 524288], P(None, ('patch', 'sub')), may hold values from -3 to 3
- area: float32 [524288], P(('patch', 'sub')), may hold values from 0.2 to 2
- corners: int32 [3, 524288], P(None, ('patch', 'sub')), may hold values from 0 to 9215, as said below
- send_sub: int32 [4096], P(('patch', 'sub')), may hold values from 0 to 8191
- send_pat: int32 [4, 4096], P(None, ('patch', 'sub')), may hold values from 0 to 8191
- live_faces: int32 [32], P(('patch', 'sub')), may hold values from 12288 to 16384, as said below
Outputs:
- divergence: float32 [262144], P(('patch', 'sub'))
The draws below stay inside these ranges and needn't reach their ends.
Inputs may be any that keep to these rules, and one draw needn't show every extreme that they name: Face slot f of a device lies in tile t = f // 128; each of its corners is either an owned position in [64 t - 128, 64 t + 128) or a remote position from 8192 + 256 (t mod (4)) up to 255 beyond that; every position of the device's table is read by some face of the device. `live_faces`: some device has all 16384 slots live.
All inputs are finite; a program needn't handle non-finite values.
Results may differ from the reference program's by a relative error of at most 0.0003.
Values sent between devices are 32-bit elements; how exact they have to be, the bound alone decides.
No kernel may reach another device: no remote copies, remote signals or barrier semaphores. Data moves between devices by JAX's collectives and lax.ppermute only.
A program may use at most 64 MiB of HBM per device.

```python
import math
import jax
import jax.numpy as jnp
from jax import lax

V_DEV = 8192
F_DEV = 16384
S_SUB = 128
S_PAT = 128
RADIUS = 2
VERTS = 262144
FACES = 524288
GROUP_SENDS = 4096
PATCH_SENDS = 4096
N_PATCH = 8
N_SUB = 4


def draw_corners(key, part):
    devices = N_PATCH * N_SUB
    remote_len = N_SUB * S_SUB + 2 * RADIUS * S_PAT
    remote_win = min(256, remote_len)
    remote_blocks = remote_len // remote_win
    tiles = F_DEV // 128
    slot = jnp.arange(F_DEV).astype(jnp.int32)
    tile = slot // 128
    inner = slot % 128

    def one_device(device_key):
        keys = jax.random.split(device_key, 6)
        tile_keys = jax.random.split(keys[0], tiles)
        orders = jax.vmap(lambda single: jax.random.permutation(single, 64))(tile_keys).astype(jnp.int32)
        first = 64 * tile + orders[tile, inner % 64]
        lower = jnp.maximum(0, 64 * (tile - 2))
        upper = jnp.minimum(V_DEV, 64 * (tile + 2))
        near_one = jax.random.randint(keys[1], (F_DEV,), lower, upper).astype(jnp.int32)
        near_two = jax.random.randint(keys[2], (F_DEV,), lower, upper).astype(jnp.int32)
        remote_order = jax.random.permutation(keys[3], remote_win).astype(jnp.int32)
        counter = tile // remote_blocks * 32 + inner // 4
        remote_base = V_DEV + remote_win * (tile % remote_blocks)
        far_one = remote_base + remote_order[counter % remote_win]
        far_two = remote_base + jax.random.randint(keys[4], (F_DEV,), 0, remote_win).astype(jnp.int32)
        flagged = jax.random.randint(keys[5], (F_DEV,), 0, 8) == 0
        second = jnp.where(inner % 4 == 0, far_one, near_one)
        third = jnp.where(flagged, far_two, near_two)
        return jnp.stack([first, second, third]).astype(jnp.int32)
    device_keys = jax.random.split(jax.random.fold_in(key, 11), devices)
    positions = jax.vmap(one_device)(device_keys)
    return positions.transpose(1, 0, 2).reshape(3, devices * F_DEV).astype(jnp.int32)


def draw_live_faces(key, part):
    devices = N_PATCH * N_SUB
    first, second = jax.random.split(jax.random.fold_in(key, 23))
    counts = jax.random.randint(first, (devices,), 3 * F_DEV // 4, F_DEV + 1).astype(jnp.int32)
    fullest = jax.random.randint(second, (), 0, devices)
    return jnp.where(jnp.arange(devices) == fullest, F_DEV, counts).astype(jnp.int32)


def place_ends(array, own_key, smallest, top_value):
    longest = array.shape.index(max(array.shape))
    spots = []
    for shift in (0, 1):
        where = [jax.random.randint(jax.random.fold_in(own_key, axis), (), 0, length) for axis, length in enumerate(array.shape)]
        where[longest] = (where[longest] + shift) % array.shape[longest]
        spots.append(tuple(where))
    return array.at[spots[0]].set(smallest).at[spots[1]].set(top_value)


def shard_levels(own_key, extent, cuts, least, top_value):
    factor_of, own = 1.0, jax.random.fold_in(own_key, 6)
    for position, shards_of in cuts:
        steps = jnp.exp(jax.random.uniform(jax.random.fold_in(own, position), (shards_of,), jnp.float32, least / len(cuts), top_value / len(cuts)))
        factor_of = factor_of * jnp.repeat(steps, extent[position] // shards_of).reshape([-1 if axis == position else 1 for axis in range(len(extent))])
    return factor_of


def centred(rng, dims, scale, bound, shards=(), dtype=jnp.bfloat16):
    level = shard_levels(rng, dims, shards, -0.22, 0.18) if shards else 1.0
    values = jax.random.normal(rng, dims, jnp.float32) * scale * level
    return jnp.minimum(jnp.maximum(values, -bound), bound).astype(dtype)


def setup_inputs(seed: int = 0) -> dict:
    splits = jax.random.split(jax.random.key(seed), 8)
    return {
        "heat": centred(splits[0], (VERTS,), 1.0, 6.0, ((0, 32),), jnp.float32),
        "basis": centred(splits[1], (9, FACES), 0.5, 3.0, ((1, 32),)),
        "area": jnp.clip(jnp.exp(math.log(2.0) - 2.3025851 * jax.random.uniform(splits[2], (FACES,), jnp.float32) ** shard_levels(splits[2], (FACES,), ((0, 32),), -0.2, 0.2)), 0.2, 2.0),
        "corners": draw_corners(jax.random.fold_in(splits[7], 71), 0),
        "send_sub": place_ends(jax.random.randint(splits[4], (GROUP_SENDS,), 0, V_DEV), jax.random.fold_in(splits[4], 1), 0, V_DEV - 1).astype(jnp.int32),
        "send_pat": place_ends(jax.random.randint(splits[5], (2 * RADIUS, PATCH_SENDS), 0, V_DEV), jax.random.fold_in(splits[5], 1), 0, V_DEV - 1).astype(jnp.int32),
        "live_faces": draw_live_faces(jax.random.fold_in(splits[7], 71), 0),
    }


def offset_list():
    return [k + 1 for k in range(RADIUS)] + [-(k + 1) for k in range(RADIUS)]

def face_terms(lookup_table, corner_ids, basis_dev, area_dev, live_count):
    slots = corner_ids.shape[1]
    values = lookup_table[corner_ids]
    gradients = basis_dev.astype(jnp.float32).reshape(3, 3, slots)
    gradient = lax.optimization_barrier(jnp.sum(gradients * values[:, None, :], axis=0))
    length = jnp.sqrt(lax.optimization_barrier(jnp.sum(gradient * gradient, axis=0)))
    field = -gradient / jnp.maximum(length, 1.0)
    projected = lax.optimization_barrier(jnp.sum(gradients * field[None, :, :], axis=1))
    live_mask = jnp.arange(slots) < live_count
    weight = jnp.where(live_mask, area_dev, 0.0)
    terms = projected * weight[None, :]
    empty = jnp.zeros((lookup_table.shape[0],), jnp.float32)
    return empty.at[corner_ids.reshape(-1)].add(terms.reshape(-1))

def reference(heat, basis, area, corners, send_sub, send_pat, live_faces):
    patch_count = N_PATCH
    sub_count = N_SUB
    devices = patch_count * sub_count
    owned_heat = heat.reshape(patch_count, sub_count, V_DEV)
    group_lists = send_sub.reshape(patch_count, sub_count, S_SUB)
    group_values = jnp.take_along_axis(owned_heat, group_lists, axis=2).reshape(patch_count, 1, sub_count * S_SUB)
    group_values = jnp.broadcast_to(group_values, (patch_count, sub_count, sub_count * S_SUB))
    patch_lists = send_pat.reshape(2 * RADIUS, patch_count, sub_count, S_PAT)
    blocks = []
    for block_index, offset in enumerate(offset_list()):
        sent = jnp.take_along_axis(owned_heat, patch_lists[block_index], axis=2)
        blocks.append(jnp.roll(sent, offset, axis=0))
    patch_values = jnp.stack(blocks, axis=2).reshape(patch_count, sub_count, 2 * RADIUS * S_PAT)
    lookup_table = jnp.concatenate([owned_heat, group_values, patch_values], axis=2)
    table_len = lookup_table.shape[2]
    lookup_table = lookup_table.reshape(devices, table_len)
    corner_ids = corners.reshape(3, devices, F_DEV).transpose(1, 0, 2)
    basis_dev = basis.reshape(9, devices, F_DEV).transpose(1, 0, 2)
    area_dev = area.reshape(devices, F_DEV)
    table_sums = lax.map(lambda pack: face_terms(*pack), (lookup_table, corner_ids, basis_dev, area_dev, live_faces))
    table_sums = table_sums.reshape(patch_count, sub_count, table_len)
    result = table_sums[:, :, :V_DEV]
    start = V_DEV
    group_sums = table_sums[:, :, start:start + sub_count * S_SUB].reshape(patch_count, sub_count, sub_count, S_SUB)
    group_sums = lax.optimization_barrier(jnp.sum(group_sums, axis=1))
    patch_ids = jnp.arange(patch_count).astype(jnp.int32)[:, None, None]
    sub_ids = jnp.arange(sub_count).astype(jnp.int32)[None, :, None]
    result = result.at[patch_ids, sub_ids, group_lists].add(group_sums)
    start = V_DEV + sub_count * S_SUB
    patch_sums = table_sums[:, :, start:].reshape(patch_count, sub_count, 2 * RADIUS, S_PAT)
    for block_index, offset in enumerate(offset_list()):
        returned = jnp.roll(patch_sums[:, :, block_index], -offset, axis=0)
        result = result.at[patch_ids, sub_ids, patch_lists[block_index]].add(returned)
    return result.reshape(-1)
```

```python
import jax
import jax.numpy as jnp
from jax import lax
from jax.experimental import pallas as pl
from jax.experimental.pallas import tpu as pltpu
from jax.sharding import PartitionSpec as P

LANES = 128
HALF = 64
VMEM = pl.BlockSpec(memory_space=pltpu.VMEM)
SMEM = pl.BlockSpec(memory_space=pltpu.SMEM)


def shift(x, axis, by):
    n = lax.axis_size(axis)
    return lax.ppermute(x, axis, [(i, (i + by) % n) for i in range(n)])


def swap(x, axis, bit):
    n = lax.axis_size(axis)
    return lax.ppermute(x, axis, [(i, i ^ bit) for i in range(n)])


def iota(shape, dim, dtype=jnp.int32):
    return lax.broadcasted_iota(jnp.int32, shape, dim).astype(dtype)


def lane_gather(table, lanes):
    return jnp.take_along_axis(table, lanes, axis=1, mode="promise_in_bounds")


def send_kernel(rows, heat_ref, sub_ref, pat_ref, out_ref):
    blocks = rows // 8
    sub_iota = iota((8, LANES), 0)
    for j in range(5):
        index = sub_ref[0:1, :] if j == 0 else pat_ref[j - 1 : j, :]
        index = jnp.broadcast_to(index, (8, LANES))
        lane = index & (LANES - 1)
        row = index >> 7
        total = jnp.zeros((8, LANES), jnp.float32)
        for a in range(blocks):
            got = lane_gather(heat_ref[8 * a : 8 * a + 8, :], lane)
            total = jnp.where(row == sub_iota + 8 * a, got, total)
        total = jnp.where((row & 7) == sub_iota, total, 0.0)
        out_ref[j : j + 1, :] = jnp.sum(total, axis=0, keepdims=True)


def faces_kernel(
    owned,
    tiles,
    blocks,
    live_ref,
    heat_ref,
    remote_ref,
    corner_ref,
    basis_ref,
    area_ref,
    own_out,
    remote_out,
    win,
    lane_s,
    half_s,
    hi_s,
    lo_s,
    sums_s,
):
    rows = owned // LANES
    live = live_ref[0]
    lane_iota = iota((8, LANES), 1)
    sub_iota = iota((8, LANES), 0)
    zero = jnp.zeros((8, LANES), jnp.float32)
    win[0:8, :] = zero
    win[2 * rows : 2 * rows + 8, :] = zero
    for a in range(rows // 8):
        here = heat_ref[8 * a : 8 * a + 8, :]
        if a + 1 < rows // 8:
            after = heat_ref[8 * a + 1 : 8 * a + 9, :]
        else:
            after = jnp.concatenate([heat_ref[8 * a + 1 : 8 * a + 8, :], zero[0:1]], axis=0)
        both = jnp.where(lane_iota < HALF, after, here)
        win[pl.ds(16 * a + 2, 8, stride=2), :] = here
        win[pl.ds(16 * a + 3, 8, stride=2), :] = pltpu.roll(both, HALF, 1)
    first = pltpu.roll(jnp.broadcast_to(heat_ref[0:1, :], (8, LANES)), HALF, 1)
    win[1:2, :] = jnp.where(lane_iota < HALF, 0.0, first)[0:1]
    remote_rows = [
        jnp.concatenate([remote_ref[2 * (t % blocks) + i : 2 * (t % blocks) + i + 1, :] for t in range(8)], axis=0)
        for i in range(2)
    ]
    half_iota = iota((HALF, LANES), 0, jnp.float32).astype(jnp.bfloat16)
    one = jnp.ones((HALF, LANES), jnp.bfloat16)
    nil = jnp.zeros((HALF, LANES), jnp.bfloat16)
    pad = jnp.zeros((16, LANES), jnp.bfloat16)

    def group(g, remote_sums):
        t0 = pl.multiple_of(8 * g, 8)
        tile = t0 + sub_iota
        near = [win[pl.ds(t0, 8), :], win[pl.ds(t0 + 2, 8), :]]
        slot = tile * LANES + lane_iota
        near_start = HALF * tile - LANES
        far_start = owned + 2 * LANES * (sub_iota % blocks)
        values, offs = [], []
        for k in range(3):
            pos = corner_ref[k, pl.ds(t0, 8), :]
            far = pos >= owned
            off = pos - jnp.where(far, far_start, near_start)
            lane = off & (LANES - 1)
            upper = off >= LANES
            got_near = jnp.where(upper, lane_gather(near[1], lane), lane_gather(near[0], lane))
            got_far = jnp.where(upper, lane_gather(remote_rows[1], lane), lane_gather(remote_rows[0], lane))
            values.append(jnp.where(far, got_far, got_near))
            offs.append(jnp.where(far, off + 2 * LANES, off))
        basis = [basis_ref[i, pl.ds(t0, 8), :].astype(jnp.float32) for i in range(9)]
        grad = [sum(basis[3 * k + c] * values[k] for k in range(3)) for c in range(3)]
        square = grad[0] * grad[0] + grad[1] * grad[1] + grad[2] * grad[2]
        scale = -area_ref[pl.ds(t0, 8), :] / jnp.maximum(jnp.sqrt(square), 1.0)
        scale = jnp.where(slot < live, scale, 0.0)
        field = [grad[c] * scale for c in range(3)]
        for k in range(3):
            term = sum(basis[3 * k + c] * field[c] for c in range(3))
            hi = term.astype(jnp.bfloat16).astype(jnp.float32)
            hi_s[k] = hi
            lo_s[k] = term - hi
            half_s[k] = offs[k] >> 6
            lane_s[k] = (offs[k] & (HALF - 1)).astype(jnp.float32)
        out = []
        for pair in range(4):
            left, right = [], []
            for t in range(2):
                for k in range(3):
                    at = pl.ds(2 * pair + t, 1)
                    half = jnp.broadcast_to(half_s[k, at, :], (8, LANES))
                    match = half == sub_iota
                    a_hi = jnp.where(match, jnp.broadcast_to(hi_s[k, at, :], (8, LANES)), 0.0)
                    a_lo = jnp.where(match, jnp.broadcast_to(lo_s[k, at, :], (8, LANES)), 0.0)
                    a = jnp.concatenate([a_hi, a_lo], axis=0).astype(jnp.bfloat16)
                    left.append(jnp.concatenate([a, pad] if t == 0 else [pad, a], axis=0))
                    lane = jnp.broadcast_to(lane_s[k, at, :], (HALF, LANES)).astype(jnp.bfloat16)
                    right.append(jnp.where(lane == half_iota, one, nil))
            product = lax.dot_general(
                jnp.concatenate(left, axis=1),
                jnp.concatenate(right, axis=1),
                (((1,), (1,)), ((), ())),
                preferred_element_type=jnp.float32,
            )
            for t in range(2):
                total = product[16 * t : 16 * t + 8] + product[16 * t + 8 : 16 * t + 16]
                sums_s[pl.ds(pl.multiple_of(8 * (t0 + 2 * pair + t), 8), 8), 0:HALF] = total
                out.append(total)
        return tuple(
            acc + sum(out[t] for t in range(8) if t % blocks == b)
            for b, acc in enumerate(remote_sums)
        )

    start = tuple(jnp.zeros((8, HALF), jnp.float32) for _ in range(blocks))
    remote_sums = lax.fori_loop(0, tiles // 8, group, start)
    for b in range(blocks):
        for i in range(2):
            both = jnp.concatenate([remote_sums[b][4 + 2 * i : 5 + 2 * i], remote_sums[b][5 + 2 * i : 6 + 2 * i]], axis=1)
            remote_out[2 * b + i : 2 * b + i + 1, :] = both
    sums_s[8 * tiles : 8 * tiles + 32, :] = jnp.zeros((32, LANES), jnp.float32)
    for a in range(rows // 8):
        parts = []
        for odd in range(2):
            total = jnp.zeros((8, LANES), jnp.float32)
            for i in range(4):
                lowest = 16 * a + odd + 2 - i
                if lowest >= 0:
                    got = sums_s[pl.ds(8 * lowest + i, 8, stride=16), :]
                else:
                    got = sums_s[pl.ds(8 * (lowest + 2) + i, 8, stride=16), :]
                    got = jnp.where(sub_iota == 0, 0.0, pltpu.roll(got, 1, 0))
                total = total + got
            parts.append(total)
        own_out[8 * a : 8 * a + 8, :] = jnp.where(lane_iota < HALF, parts[0], pltpu.roll(parts[1], HALF, 1))


def faces_call(live_faces, heat2, remote, corners, basis, area):
    rows = heat2.shape[0]
    tiles = corners.shape[1] // LANES
    blocks = remote.shape[0] // 2
    return pl.pallas_call(
        lambda *refs: faces_kernel(rows * LANES, tiles, blocks, *refs),
        out_shape=(
            jax.ShapeDtypeStruct((rows, LANES), jnp.float32),
            jax.ShapeDtypeStruct((2 * blocks, LANES), jnp.float32),
        ),
        in_specs=[SMEM] + [VMEM] * 5,
        out_specs=(VMEM, VMEM),
        scratch_shapes=[
            pltpu.VMEM((2 * rows + 8, LANES), jnp.float32),
            pltpu.VMEM((3, 8, LANES), jnp.float32),
            pltpu.VMEM((3, 8, LANES), jnp.int32),
            pltpu.VMEM((3, 8, LANES), jnp.float32),
            pltpu.VMEM((3, 8, LANES), jnp.float32),
            pltpu.VMEM((8 * tiles + 128, LANES), jnp.float32),
        ],
        name="faces",
    )(
        live_faces,
        heat2,
        remote,
        corners.reshape(3, tiles, LANES),
        basis.reshape(9, tiles, LANES),
        area.reshape(tiles, LANES),
    )


def scatter_kernel(rows, own_ref, back_ref, sub_ref, pat_ref, out_ref):
    row_iota = iota((rows, LANES), 0)
    lane_iota = iota((LANES, LANES), 0)
    left, right = [], []
    for j in range(5):
        index = sub_ref[0:1, :] if j == 0 else pat_ref[j - 1 : j, :]
        value = back_ref[j : j + 1, :]
        hi = value.astype(jnp.bfloat16).astype(jnp.float32)
        match = jnp.broadcast_to(index >> 7, (rows, LANES)) == row_iota
        a_hi = jnp.where(match, jnp.broadcast_to(hi, (rows, LANES)), 0.0)
        a_lo = jnp.where(match, jnp.broadcast_to(value - hi, (rows, LANES)), 0.0)
        left.append(jnp.concatenate([a_hi, a_lo], axis=0).astype(jnp.bfloat16))
        spot = jnp.broadcast_to(index & (LANES - 1), (LANES, LANES)) == lane_iota
        right.append(jnp.where(spot, 1.0, 0.0).astype(jnp.bfloat16))
    product = lax.dot_general(
        jnp.concatenate(left, axis=1),
        jnp.concatenate(right, axis=1),
        (((1,), (1,)), ((), ())),
        preferred_element_type=jnp.float32,
    )
    out_ref[...] = own_ref[...] + product[:rows] + product[rows:]


def per_device(heat, basis, area, corners, send_sub, send_pat, live_faces):
    owned = heat.shape[0]
    slots = corners.shape[1]
    tiles = slots // LANES
    rows = owned // LANES
    group = lax.axis_size("sub")
    group_size = send_sub.shape[0]
    block_size = send_pat.shape[1]
    offsets = send_pat.shape[0]
    remote_len = group * group_size + offsets * block_size
    blocks = remote_len // (2 * LANES)
    assert offsets == 4 and block_size == LANES and group_size <= LANES
    assert group & (group - 1) == 0 and 8 % blocks == 0 and remote_len == 2 * LANES * blocks
    odd = lax.axis_index("patch") % 2 == 1
    me = lax.axis_index("sub")
    heat2 = heat.reshape(rows, LANES)
    sub2 = jnp.pad(send_sub, (0, LANES - group_size)).reshape(1, LANES)

    sent = pl.pallas_call(
        lambda *refs: send_kernel(rows, *refs),
        out_shape=jax.ShapeDtypeStruct((5, LANES), jnp.float32),
        in_specs=[VMEM, VMEM, VMEM],
        out_specs=VMEM,
        name="send_gather",
    )(heat2, sub2, send_pat)

    near_first = jnp.where(odd, sent[jnp.array([3, 1])], sent[jnp.array([1, 3])])
    direct = swap(near_first, "patch", 1)
    relay = direct[1:2]
    up = shift(jnp.concatenate([sent[2:3], relay]), "patch", 2)
    down = shift(jnp.concatenate([sent[4:5], relay]), "patch", -2)
    from_below = jnp.where(odd, direct[0], up[1])
    from_above = jnp.where(odd, down[1], direct[0])
    values = sent[0:1, :group_size]
    bit = 1
    while bit < group:
        values = jnp.concatenate([values, swap(values, "sub", bit)], axis=0)
        bit = bit * 2
    order = me ^ jnp.arange(group)
    group_values = values[order].reshape(-1)
    remote = jnp.concatenate([group_values, from_below, up[0], from_above, down[0]]).reshape(2 * blocks, LANES)

    own_sums, remote_sums = faces_call(live_faces, heat2, remote, corners, basis, area)

    flat = remote_sums.reshape(-1)
    patch_sums = flat[group * group_size :].reshape(4, LANES)
    near_first = jnp.where(odd, patch_sums[jnp.array([0, 2])], patch_sums[jnp.array([2, 0])])
    direct = swap(near_first, "patch", 1)
    relay = direct[1:2]
    down = shift(jnp.concatenate([patch_sums[1:2], relay]), "patch", -2)
    up = shift(jnp.concatenate([patch_sums[3:4], relay]), "patch", 2)
    back_above = jnp.where(odd, down[1], direct[0])
    back_below = jnp.where(odd, direct[0], up[1])
    group_sums = flat[: group * group_size].reshape(group, group_size)[order]
    bit = group // 2
    while bit >= 1:
        group_sums = group_sums[:bit] + swap(group_sums[bit:], "sub", bit)
        bit = bit // 2
    group_back = jnp.pad(group_sums, ((0, 0), (0, LANES - group_size)))
    back = jnp.concatenate([group_back, jnp.stack([back_above, down[0], back_below, up[0]])])

    result = pl.pallas_call(
        lambda *refs: scatter_kernel(rows, *refs),
        out_shape=jax.ShapeDtypeStruct((rows, LANES), jnp.float32),
        in_specs=[VMEM] * 4,
        out_specs=VMEM,
        name="scatter_back",
    )(own_sums, back, sub2, send_pat)
    return result.reshape(-1)


def solution(mesh):
    placed = (
        P(("patch", "sub")),
        P(None, ("patch", "sub")),
        P(("patch", "sub")),
        P(None, ("patch", "sub")),
        P(("patch", "sub")),
        P(None, ("patch", "sub")),
        P(("patch", "sub")),
    )
    return jax.shard_map(
        per_device, mesh=mesh, in_specs=placed, out_specs=P(("patch", "sub")), check_vma=False
    )
```

```python
import jax
import jax.numpy as jnp
from jax import lax
from jax.experimental import pallas as pl
from jax.experimental.pallas import tpu as pltpu
from jax.sharding import PartitionSpec as P

LANES = 128
HALF = 64
VMEM = pl.BlockSpec(memory_space=pltpu.VMEM)
SMEM = pl.BlockSpec(memory_space=pltpu.SMEM)


def shift(x, axis, by):
    n = lax.axis_size(axis)
    return lax.ppermute(x, axis, [(i, (i + by) % n) for i in range(n)])


def swap(x, axis, bit):
    n = lax.axis_size(axis)
    return lax.ppermute(x, axis, [(i, i ^ bit) for i in range(n)])


def iota(shape, dim, dtype=jnp.int32):
    return lax.broadcasted_iota(jnp.int32, shape, dim).astype(dtype)


def lane_gather(table, lanes):
    return jnp.take_along_axis(table, lanes, axis=1, mode="promise_in_bounds")


def read(ref, at):
    return ref[pl.ds(at, 1), :]


def send_kernel(rows, heat_ref, sub_ref, pat_ref, group_ref, near_ref, up_ref, down_ref):
    blocks = rows // 8
    sub_iota = iota((8, LANES), 0)
    odd = lax.axis_index("patch") & 1
    for j in range(5):
        if j == 0:
            index = sub_ref[0:1, :]
        else:
            index = read(pat_ref, (1, 3, 2 * odd, 2 - 2 * odd)[j - 1])
        index = jnp.broadcast_to(index, (8, index.shape[1]))
        if index.shape[1] < LANES:
            index = jnp.concatenate([index] * (LANES // index.shape[1]), axis=1)
        lane = index & (LANES - 1)
        row = index >> 7
        total = jnp.zeros((8, LANES), jnp.float32)
        for a in range(blocks):
            got = lane_gather(heat_ref[8 * a : 8 * a + 8, :], lane)
            total = jnp.where(row == sub_iota + 8 * a, got, total)
        total = jnp.where((row & 7) == sub_iota, total, 0.0)
        total = jnp.sum(total, axis=0, keepdims=True)
        if j == 0:
            group_ref[...] = total[:, : sub_ref.shape[1]]
        elif j < 3:
            (up_ref, down_ref)[j - 1][...] = total
        else:
            near_ref[j - 3 : j - 2, :] = total


def faces_kernel(
    owned,
    tiles,
    blocks,
    group,
    live_ref,
    heat_ref,
    corner_ref,
    basis_ref,
    area_ref,
    direct_ref,
    up_ref,
    down_ref,
    *refs,
):
    bits = group.bit_length() - 1
    group_refs = refs[: bits + 1]
    own_out, group_keep, *group_outs, near_out, up_out, down_out = refs[bits + 1 : 2 * bits + 6]
    win, lane_s, half_s, hi_s, lo_s, sums_s, remote_ref, remote_out = refs[2 * bits + 6 :]
    group_size = group_keep.shape[1]
    odd = lax.axis_index("patch") & 1
    me = lax.axis_index("sub")
    per_row = LANES // group_size
    for q in range(group // per_row):
        parts = []
        for e in range(per_row):
            from_me = me ^ (q * per_row + e)
            part = group_refs[0][...]
            for bit in range(bits):
                got = read(group_refs[bit + 1], from_me & ((1 << bit) - 1))
                part = jnp.where(from_me >> bit == 1, got, part)
            parts.append(part)
        remote_ref[q : q + 1, :] = parts[0] if per_row == 1 else jnp.concatenate(parts, axis=1)
    base = group // per_row
    is_odd = jnp.broadcast_to(odd, (1, LANES)) == 1
    direct = direct_ref[0:1, :]
    remote_ref[base : base + 1, :] = jnp.where(is_odd, direct, up_ref[1:2, :])
    remote_ref[base + 1 : base + 2, :] = up_ref[0:1, :]
    remote_ref[base + 2 : base + 3, :] = jnp.where(is_odd, down_ref[1:2, :], direct)
    remote_ref[base + 3 : base + 4, :] = down_ref[0:1, :]
    rows = owned // LANES
    live = live_ref[0]
    lane_iota = iota((8, LANES), 1)
    sub_iota = iota((8, LANES), 0)
    zero = jnp.zeros((8, LANES), jnp.float32)
    win[0:8, :] = zero
    win[2 * rows : 2 * rows + 8, :] = zero
    for a in range(rows // 8):
        here = heat_ref[8 * a : 8 * a + 8, :]
        if a + 1 < rows // 8:
            after = heat_ref[8 * a + 1 : 8 * a + 9, :]
        else:
            after = jnp.concatenate([heat_ref[8 * a + 1 : 8 * a + 8, :], zero[0:1]], axis=0)
        both = jnp.where(lane_iota < HALF, after, here)
        win[pl.ds(16 * a + 2, 8, stride=2), :] = here
        win[pl.ds(16 * a + 3, 8, stride=2), :] = pltpu.roll(both, HALF, 1)
    first = pltpu.roll(jnp.broadcast_to(heat_ref[0:1, :], (8, LANES)), HALF, 1)
    win[1:2, :] = jnp.where(lane_iota < HALF, 0.0, first)[0:1]
    remote_rows = [
        jnp.concatenate([remote_ref[2 * (t % blocks) + i : 2 * (t % blocks) + i + 1, :] for t in range(8)], axis=0)
        for i in range(2)
    ]
    half_iota = iota((HALF, LANES), 0, jnp.float32).astype(jnp.bfloat16)
    one = jnp.ones((HALF, LANES), jnp.bfloat16)
    nil = jnp.zeros((HALF, LANES), jnp.bfloat16)
    pad = jnp.zeros((16, LANES), jnp.bfloat16)

    def eight_tiles(g, remote_sums):
        t0 = pl.multiple_of(8 * g, 8)
        tile = t0 + sub_iota
        near = [win[pl.ds(t0, 8), :], win[pl.ds(t0 + 2, 8), :]]
        slot = tile * LANES + lane_iota
        near_start = HALF * tile - LANES
        far_start = owned + 2 * LANES * (sub_iota % blocks)
        values, offs = [], []
        for k in range(3):
            pos = corner_ref[k, pl.ds(t0, 8), :]
            far = pos >= owned
            off = pos - jnp.where(far, far_start, near_start)
            lane = off & (LANES - 1)
            upper = off >= LANES
            got_near = jnp.where(upper, lane_gather(near[1], lane), lane_gather(near[0], lane))
            got_far = jnp.where(upper, lane_gather(remote_rows[1], lane), lane_gather(remote_rows[0], lane))
            values.append(jnp.where(far, got_far, got_near))
            offs.append(jnp.where(far, off + 2 * LANES, off))
        basis = [basis_ref[i, pl.ds(t0, 8), :].astype(jnp.float32) for i in range(9)]
        grad = [sum(basis[3 * k + c] * values[k] for k in range(3)) for c in range(3)]
        square = grad[0] * grad[0] + grad[1] * grad[1] + grad[2] * grad[2]
        scale = -area_ref[pl.ds(t0, 8), :] / jnp.maximum(jnp.sqrt(square), 1.0)
        scale = jnp.where(slot < live, scale, 0.0)
        field = [grad[c] * scale for c in range(3)]
        for k in range(3):
            term = sum(basis[3 * k + c] * field[c] for c in range(3))
            hi = term.astype(jnp.bfloat16).astype(jnp.float32)
            hi_s[k] = hi
            lo_s[k] = term - hi
            half_s[k] = offs[k] >> 6
            lane_s[k] = (offs[k] & (HALF - 1)).astype(jnp.float32)
        out = []
        for pair in range(4):
            left, right = [], []
            for t in range(2):
                for k in range(3):
                    at = pl.ds(2 * pair + t, 1)
                    half = jnp.broadcast_to(half_s[k, at, :], (8, LANES))
                    match = half == sub_iota
                    a_hi = jnp.where(match, jnp.broadcast_to(hi_s[k, at, :], (8, LANES)), 0.0)
                    a_lo = jnp.where(match, jnp.broadcast_to(lo_s[k, at, :], (8, LANES)), 0.0)
                    a = jnp.concatenate([a_hi, a_lo], axis=0).astype(jnp.bfloat16)
                    left.append(jnp.concatenate([a, pad] if t == 0 else [pad, a], axis=0))
                    lane = jnp.broadcast_to(lane_s[k, at, :], (HALF, LANES)).astype(jnp.bfloat16)
                    right.append(jnp.where(lane == half_iota, one, nil))
            product = lax.dot_general(
                jnp.concatenate(left, axis=1),
                jnp.concatenate(right, axis=1),
                (((1,), (1,)), ((), ())),
                preferred_element_type=jnp.float32,
            )
            for t in range(2):
                total = product[16 * t : 16 * t + 8] + product[16 * t + 8 : 16 * t + 16]
                sums_s[pl.ds(pl.multiple_of(8 * (t0 + 2 * pair + t), 8), 8), 0:HALF] = total
                out.append(total)
        return tuple(
            acc + sum(out[t] for t in range(8) if t % blocks == b)
            for b, acc in enumerate(remote_sums)
        )

    start = tuple(jnp.zeros((8, HALF), jnp.float32) for _ in range(blocks))
    remote_sums = lax.fori_loop(0, tiles // 8, eight_tiles, start)
    for b in range(blocks):
        for i in range(2):
            both = jnp.concatenate([remote_sums[b][4 + 2 * i : 5 + 2 * i], remote_sums[b][5 + 2 * i : 6 + 2 * i]], axis=1)
            remote_out[2 * b + i : 2 * b + i + 1, :] = both
    up_out[...] = remote_out[base + 3 : base + 4, :]
    down_out[...] = remote_out[base + 1 : base + 2, :]
    near_out[0:1, :] = read(remote_out, base + 2 - 2 * odd)
    near_out[1:2, :] = read(remote_out, base + 2 * odd)
    for i in range(group):
        owner = me ^ i
        if per_row == 1:
            row = read(remote_out, owner)
        else:
            row = read(remote_out, owner // per_row)
            row = pltpu.roll(jnp.broadcast_to(row, (8, LANES)), (LANES - (owner % per_row) * group_size) % LANES, 1)[0:1, :group_size]
        if i == 0:
            group_keep[...] = row
        else:
            bit = i.bit_length() - 1
            group_outs[bit][i - (1 << bit) : i - (1 << bit) + 1, :] = row
    sums_s[8 * tiles : 8 * tiles + 32, :] = jnp.zeros((32, LANES), jnp.float32)
    for a in range(rows // 8):
        parts = []
        for odd in range(2):
            total = jnp.zeros((8, LANES), jnp.float32)
            for i in range(4):
                lowest = 16 * a + odd + 2 - i
                if lowest >= 0:
                    got = sums_s[pl.ds(8 * lowest + i, 8, stride=16), :]
                else:
                    got = sums_s[pl.ds(8 * (lowest + 2) + i, 8, stride=16), :]
                    got = jnp.where(sub_iota == 0, 0.0, pltpu.roll(got, 1, 0))
                total = total + got
            parts.append(total)
        own_out[8 * a : 8 * a + 8, :] = jnp.where(lane_iota < HALF, parts[0], pltpu.roll(parts[1], HALF, 1))


def faces_call(live_faces, heat2, corners, basis, area, group, group_size, received):
    rows = heat2.shape[0]
    tiles = corners.shape[1] // LANES
    bits = group.bit_length() - 1
    blocks = (group * group_size + 4 * LANES) // (2 * LANES)
    f32 = jnp.float32
    group_rows = [1] + [1 << bit for bit in range(bits)]
    return pl.pallas_call(
        lambda *refs: faces_kernel(rows * LANES, tiles, blocks, group, *refs),
        out_shape=(
            jax.ShapeDtypeStruct((rows, LANES), f32),
            *[jax.ShapeDtypeStruct((n, group_size), f32) for n in group_rows],
            jax.ShapeDtypeStruct((2, LANES), f32),
            jax.ShapeDtypeStruct((1, LANES), f32),
            jax.ShapeDtypeStruct((1, LANES), f32),
        ),
        in_specs=[SMEM] + [VMEM] * (4 + len(received)),
        out_specs=(VMEM,) * (bits + 5),
        scratch_shapes=[
            pltpu.VMEM((2 * rows + 8, LANES), f32),
            pltpu.VMEM((3, 8, LANES), f32),
            pltpu.VMEM((3, 8, LANES), jnp.int32),
            pltpu.VMEM((3, 8, LANES), f32),
            pltpu.VMEM((3, 8, LANES), f32),
            pltpu.VMEM((8 * tiles + 128, LANES), f32),
            pltpu.VMEM((2 * blocks, LANES), f32),
            pltpu.VMEM((2 * blocks, LANES), f32),
        ],
        compiler_params=pltpu.CompilerParams(vmem_limit_bytes=6 * 2**20),
        name="faces",
    )(
        live_faces,
        heat2,
        corners.reshape(3, tiles, LANES),
        basis.reshape(9, tiles, LANES),
        area.reshape(tiles, LANES),
        *received,
    )


def scatter_kernel(rows, bits, own_ref, sub_ref, pat_ref, direct_ref, up_ref, down_ref, *refs):
    out_ref = refs[-1]
    row_iota = iota((rows, LANES), 0)
    lane_iota = iota((LANES, LANES), 0)
    odd = jnp.broadcast_to(lax.axis_index("patch") & 1, (1, LANES)) == 1
    direct = direct_ref[0:1, :]
    group_back = refs[0][...]
    for i in range(bits):
        ref = refs[i + 1]
        for at in range(0, ref.shape[0], 1 << (bits - 1 - i)):
            group_back = group_back + ref[at : at + 1, :]
    backs = [
        group_back,
        jnp.where(odd, down_ref[1:2, :], direct),
        down_ref[0:1, :],
        jnp.where(odd, direct, up_ref[1:2, :]),
        up_ref[0:1, :],
    ]
    left, right = [], []
    for j in range(5):
        index = sub_ref[0:1, :] if j == 0 else pat_ref[j - 1 : j, :]
        value = backs[j]
        width = index.shape[1]
        hi = value.astype(jnp.bfloat16).astype(jnp.float32)
        match = jnp.broadcast_to(index >> 7, (rows, width)) == row_iota[:, :width]
        a_hi = jnp.where(match, jnp.broadcast_to(hi, (rows, width)), 0.0)
        a_lo = jnp.where(match, jnp.broadcast_to(value - hi, (rows, width)), 0.0)
        left.append(jnp.concatenate([a_hi, a_lo], axis=0).astype(jnp.bfloat16))
        spot = jnp.broadcast_to(index & (LANES - 1), (LANES, width)) == lane_iota[:, :width]
        right.append(jnp.where(spot, 1.0, 0.0).astype(jnp.bfloat16))
    product = 0.0
    for part in ([0], [1, 2, 3, 4]) if left[0].shape[1] < LANES else ([0, 1, 2, 3, 4],):
        product = product + lax.dot_general(
            jnp.concatenate([left[j] for j in part], axis=1),
            jnp.concatenate([right[j] for j in part], axis=1),
            (((1,), (1,)), ((), ())),
            preferred_element_type=jnp.float32,
        )
    out_ref[...] = own_ref[...] + product[:rows] + product[rows:]


def stack(parts):
    return parts[0] if len(parts) == 1 else jnp.concatenate(parts, axis=0)


def per_device(heat, basis, area, corners, send_sub, send_pat, live_faces):
    owned = heat.shape[0]
    rows = owned // LANES
    group = lax.axis_size("sub")
    group_size = send_sub.shape[0]
    block_size = send_pat.shape[1]
    offsets = send_pat.shape[0]
    remote_len = group * group_size + offsets * block_size
    assert offsets == 4 and block_size == LANES and LANES % group_size == 0
    assert group & (group - 1) == 0 and remote_len in (512, 1024, 2048)
    assert lax.axis_size("patch") % 2 == 0
    bits = group.bit_length() - 1
    f32 = jnp.float32
    heat2 = heat.reshape(rows, LANES)
    sub2 = send_sub.reshape(1, group_size)

    mine, near, up, down = pl.pallas_call(
        lambda *refs: send_kernel(rows, *refs),
        out_shape=(
            jax.ShapeDtypeStruct((1, group_size), f32),
            jax.ShapeDtypeStruct((2, LANES), f32),
            jax.ShapeDtypeStruct((1, LANES), f32),
            jax.ShapeDtypeStruct((1, LANES), f32),
        ),
        in_specs=[VMEM, VMEM, VMEM],
        out_specs=(VMEM,) * 4,
        compiler_params=pltpu.CompilerParams(vmem_limit_bytes=2 * 2**20),
        name="send_gather",
    )(heat2, sub2, send_pat)
    direct = swap(near, "patch", 1)
    relay = direct[1:2]
    from_below = shift(jnp.concatenate([up, relay]), "patch", 2)
    from_above = shift(jnp.concatenate([down, relay]), "patch", -2)
    held = [mine]
    for bit in range(bits):
        held.append(swap(stack(held), "sub", 1 << bit))

    own_sums, keep, *outs, near, up, down = faces_call(
        live_faces, heat2, corners, basis, area, group, group_size,
        (direct, from_below, from_above, *held),
    )

    direct = swap(near, "patch", 1)
    relay = direct[1:2]
    from_above = shift(jnp.concatenate([down, relay]), "patch", -2)
    from_below = shift(jnp.concatenate([up, relay]), "patch", 2)
    pieces, group_back = [], []
    for bit in reversed(range(bits)):
        width = 1 << bit
        got = swap(stack([outs[bit]] + [p[width : 2 * width] for p in pieces]), "sub", width)
        group_back.append(got)
        pieces = [p[:width] for p in pieces] + [
            got[at : at + width] for at in range(0, got.shape[0], width)
        ]

    result = pl.pallas_call(
        lambda *refs: scatter_kernel(rows, bits, *refs),
        out_shape=jax.ShapeDtypeStruct((rows, LANES), f32),
        in_specs=[VMEM] * (7 + bits),
        out_specs=VMEM,
        compiler_params=pltpu.CompilerParams(vmem_limit_bytes=4 * 2**20),
        name="scatter_back",
    )(own_sums, sub2, send_pat, direct, from_below, from_above, keep, *group_back)
    return result.reshape(-1)


def solution(mesh):
    placed = (
        P(("patch", "sub")),
        P(None, ("patch", "sub")),
        P(("patch", "sub")),
        P(None, ("patch", "sub")),
        P(("patch", "sub")),
        P(None, ("patch", "sub")),
        P(("patch", "sub")),
    )
    return jax.shard_map(
        per_device, mesh=mesh, in_specs=placed, out_specs=P(("patch", "sub")), check_vma=False
    )
```

```python
import jax
import jax.numpy as jnp
from jax import lax
from jax.experimental import pallas as pl
from jax.experimental.pallas import tpu as pltpu
from jax.sharding import PartitionSpec as P


LANES = 128
HALF = 64
UNROLL = (8, 4, 4)
COST = (1 << 24, 1 << 24)
VMEM = pl.BlockSpec(memory_space=pltpu.VMEM)
HBM = pl.BlockSpec(memory_space=pltpu.HBM)
SMEM = pl.BlockSpec(memory_space=pltpu.SMEM)


def shift(x, axis, by):
    n = lax.axis_size(axis)
    return lax.ppermute(x, axis, [(i, (i + by) % n) for i in range(n)])


def swap(x, axis, bit):
    n = lax.axis_size(axis)
    return lax.ppermute(x, axis, [(i, i ^ bit) for i in range(n)])


def iota(shape, dim, dtype=jnp.int32):
    return lax.broadcasted_iota(jnp.int32, shape, dim).astype(dtype)


def lane_gather(table, lanes):
    return jnp.take_along_axis(table, lanes, axis=1, mode="promise_in_bounds")


def read(ref, at):
    return ref[pl.ds(at, 1), :]


def send_kernel(
    rows, heat_hbm, sub_hbm, pat_hbm, group_ref, near_ref, up_ref, down_ref, sub_ref, pat_ref, heat_ref, sems
):
    copies = [
        pltpu.make_async_copy(source, target, sems.at[i])
        for i, (source, target) in enumerate(((heat_hbm, heat_ref), (sub_hbm, sub_ref), (pat_hbm, pat_ref)))
    ]
    for copy in copies:
        copy.start()
    for copy in copies:
        copy.wait()
    blocks = rows // 8
    sub_iota = iota((8, LANES), 0)
    odd = lax.axis_index("patch") & 1
    for j in range(5):
        if j == 0:
            index = sub_ref[0:1, :]
        else:
            index = read(pat_ref, (1, 3, 2 * odd, 2 - 2 * odd)[j - 1])
        index = jnp.broadcast_to(index, (8, index.shape[1]))
        if index.shape[1] < LANES:
            index = jnp.concatenate([index] * (LANES // index.shape[1]), axis=1)
        lane = index & (LANES - 1)
        row = index >> 7
        total = jnp.zeros((8, LANES), jnp.float32)
        for a in range(blocks):
            got = lane_gather(heat_ref[8 * a : 8 * a + 8, :], lane)
            total = jnp.where(row == sub_iota + 8 * a, got, total)
        total = jnp.where((row & 7) == sub_iota, total, 0.0)
        total = jnp.sum(total, axis=0, keepdims=True)
        if j == 0:
            group_ref[...] = total[:, : sub_ref.shape[1]]
        elif j < 3:
            (up_ref, down_ref)[j - 1][...] = total
        else:
            near_ref[j - 3 : j - 2, :] = total


def prepare_kernel(
    owned,
    tiles,
    blocks,
    live_ref,
    heat_hbm,
    corner_hbm,
    basis_hbm,
    area_hbm,
    near_out,
    off_out,
    half_out,
    lane_out,
    basis_out,
    last_out,
    weight_out,
    heat_ref,
    corner_ref,
    basis_ref,
    win,
    corner_s,
    sems,
):
    copies = [
        pltpu.make_async_copy(source, target, sems.at[i])
        for i, (source, target) in enumerate(
            ((corner_hbm, corner_ref), (heat_hbm, heat_ref), (basis_hbm, basis_ref), (area_hbm, weight_out))
        )
    ]
    for copy in copies:
        copy.start()
    rows = owned // LANES
    lane_iota = iota((8, LANES), 1)
    sub_iota = iota((8, LANES), 0)
    copies[1].wait()
    zero = jnp.zeros((8, LANES), jnp.float32)
    win[0:8, :] = zero
    win[2 * rows : 2 * rows + 8, :] = zero
    for a in range(rows // 8):
        here = heat_ref[8 * a : 8 * a + 8, :]
        if a + 1 < rows // 8:
            after = heat_ref[8 * a + 1 : 8 * a + 9, :]
        else:
            after = jnp.concatenate([heat_ref[8 * a + 1 : 8 * a + 8, :], zero[0:1]], axis=0)
        both = jnp.where(lane_iota < HALF, after, here)
        win[pl.ds(16 * a + 2, 8, stride=2), :] = here
        win[pl.ds(16 * a + 3, 8, stride=2), :] = pltpu.roll(both, HALF, 1)
    first = pltpu.roll(jnp.broadcast_to(heat_ref[0:1, :], (8, LANES)), HALF, 1)
    win[1:2, :] = jnp.where(lane_iota < HALF, 0.0, first)[0:1]
    copies[0].wait()

    def spread_corners(t, carry):
        at = pl.ds(pl.multiple_of(LANES * t, LANES), LANES)
        corner_s[pl.ds(pl.multiple_of(4 * t, 4), 3), :] = corner_ref[:, at]
        return carry

    lax.fori_loop(0, tiles, spread_corners, 0, unroll=UNROLL[0])

    def near_values(g, carry):
        t0 = pl.multiple_of(8 * g, 8)
        tile = t0 + sub_iota
        near = [win[pl.ds(t0, 8), :], win[pl.ds(t0 + 2, 8), :]]
        near_start = HALF * tile - LANES
        far_start = owned + 2 * LANES * (sub_iota % blocks) - 2 * LANES
        at = pl.ds(t0, 8)
        for k in range(3):
            pos = corner_s[pl.ds(4 * t0 + k, 8, stride=4), :]
            off = pos - jnp.where(pos >= owned, far_start, near_start)
            lane = off & (LANES - 1)
            near_out[k, at, :] = jnp.where(
                off >= LANES, lane_gather(near[1], lane), lane_gather(near[0], lane)
            )
            off_out[k, at, :] = off
            half_out[k, at, :] = off >> 6
            lane_out[k, at, :] = (off & (HALF - 1)).astype(jnp.float32)
        return carry

    lax.fori_loop(0, tiles // 8, near_values, 0, unroll=UNROLL[1])
    copies[2].wait()

    def spread_basis(t, carry):
        at = pl.ds(pl.multiple_of(LANES * t, LANES), LANES)
        nine = basis_ref[:, at].astype(jnp.float32)
        basis_out[pl.ds(pl.multiple_of(8 * t, 8), 8), :] = nine[0:8]
        last_out[pl.ds(t, 1), :] = nine[8:9]
        return carry

    lax.fori_loop(0, tiles, spread_basis, 0, unroll=UNROLL[0])
    copies[3].wait()
    live = live_ref[0]
    for t0 in range(0, tiles, 8):
        slot = (t0 + sub_iota) * LANES + lane_iota
        weight_out[t0 : t0 + 8, :] = jnp.where(slot < live, -weight_out[t0 : t0 + 8, :], 0.0)


def prepare_call(live_faces, heat2, corners, basis, area, blocks):
    rows = heat2.shape[0]
    tiles = corners.shape[1] // LANES
    f32 = jnp.float32
    per_corner = (3, tiles, LANES)
    return pl.pallas_call(
        lambda *refs: prepare_kernel(rows * LANES, tiles, blocks, *refs),
        out_shape=(
            jax.ShapeDtypeStruct(per_corner, f32),
            jax.ShapeDtypeStruct(per_corner, jnp.int32),
            jax.ShapeDtypeStruct(per_corner, jnp.int32),
            jax.ShapeDtypeStruct(per_corner, f32),
            jax.ShapeDtypeStruct((8 * tiles, LANES), f32),
            jax.ShapeDtypeStruct((tiles, LANES), f32),
            jax.ShapeDtypeStruct((tiles, LANES), f32),
        ),
        in_specs=[SMEM] + [HBM] * 4,
        out_specs=(VMEM,) * 7,
        scratch_shapes=[
            pltpu.VMEM(heat2.shape, f32),
            pltpu.VMEM(corners.shape, jnp.int32),
            pltpu.VMEM(basis.shape, basis.dtype),
            pltpu.VMEM((2 * rows + 8, LANES), f32),
            pltpu.VMEM((4 * tiles, LANES), jnp.int32),
            pltpu.SemaphoreType.DMA((4,)),
        ],
        cost_estimate=pl.CostEstimate(flops=COST[0], bytes_accessed=1 << 20, transcendentals=0),
        compiler_params=pltpu.CompilerParams(vmem_limit_bytes=6 * 2**20),
        name="prepare",
    )(live_faces, *in_hbm(heat2, corners, basis, area.reshape(tiles, LANES)))


def faces_kernel(tiles, blocks, group, *refs):
    near_ref, off_ref, half_s, lane_s, basis_s, last_s, weight_ref, direct_ref, up_ref, down_ref, *refs = refs
    bits = group.bit_length() - 1
    group_refs = refs[: bits + 1]
    own_out, group_keep, *group_outs, near_out, up_out, down_out = refs[bits + 1 : 2 * bits + 6]
    hi_s, lo_s, sums_s, remote_ref, remote_out = refs[2 * bits + 6 :]
    group_size = group_keep.shape[1]
    odd = lax.axis_index("patch") & 1
    me = lax.axis_index("sub")
    rows = own_out.shape[0]
    lane_iota = iota((8, LANES), 1)
    sub_iota = iota((8, LANES), 0)
    per_row = LANES // group_size
    for q in range(group // per_row):
        parts = []
        for e in range(per_row):
            from_me = me ^ (q * per_row + e)
            part = group_refs[0][...]
            for bit in range(bits):
                got = read(group_refs[bit + 1], from_me & ((1 << bit) - 1))
                part = jnp.where(from_me >> bit == 1, got, part)
            parts.append(part)
        remote_ref[q : q + 1, :] = parts[0] if per_row == 1 else jnp.concatenate(parts, axis=1)
    base = group // per_row
    is_odd = jnp.broadcast_to(odd, (1, LANES)) == 1
    direct = direct_ref[0:1, :]
    remote_ref[base : base + 1, :] = jnp.where(is_odd, direct, up_ref[1:2, :])
    remote_ref[base + 1 : base + 2, :] = up_ref[0:1, :]
    remote_ref[base + 2 : base + 3, :] = jnp.where(is_odd, down_ref[1:2, :], direct)
    remote_ref[base + 3 : base + 4, :] = down_ref[0:1, :]
    remote_rows = [
        jnp.concatenate([remote_ref[2 * (t % blocks) + i : 2 * (t % blocks) + i + 1, :] for t in range(8)], axis=0)
        for i in range(2)
    ]
    half_iota = iota((HALF, LANES), 0, jnp.float32).astype(jnp.bfloat16)
    one = jnp.ones((HALF, LANES), jnp.bfloat16)
    nil = jnp.zeros((HALF, LANES), jnp.bfloat16)
    pad = jnp.zeros((16, LANES), jnp.bfloat16)

    def face_values(g, carry):
        t0 = pl.multiple_of(8 * g, 8)
        at = pl.ds(t0, 8)
        values = []
        for k in range(3):
            off = off_ref[k, at, :]
            lane = off & (LANES - 1)
            far = jnp.where(
                off >= 3 * LANES, lane_gather(remote_rows[1], lane), lane_gather(remote_rows[0], lane)
            )
            values.append(jnp.where(off >= 2 * LANES, far, near_ref[k, at, :]))
        basis = [basis_s[pl.ds(8 * t0 + i, 8, stride=8), :] for i in range(8)] + [last_s[at, :]]
        grad = [sum(basis[3 * k + c] * values[k] for k in range(3)) for c in range(3)]
        square = grad[0] * grad[0] + grad[1] * grad[1] + grad[2] * grad[2]
        scale = weight_ref[at, :] / jnp.maximum(jnp.sqrt(square), 1.0)
        field = [grad[c] * scale for c in range(3)]
        for k in range(3):
            term = sum(basis[3 * k + c] * field[c] for c in range(3))
            hi = term.astype(jnp.bfloat16).astype(jnp.float32)
            hi_s[k, at, :] = hi
            lo_s[k, at, :] = term - hi
        return carry

    lax.fori_loop(0, tiles // 8, face_values, 0, unroll=UNROLL[1])

    def eight_tiles(g, remote_sums):
        t0 = pl.multiple_of(8 * g, 8)
        out = []
        for pair in range(4):
            left, right = [], []
            for t in range(2):
                for k in range(3):
                    at = pl.ds(t0 + 2 * pair + t, 1)
                    half = jnp.broadcast_to(half_s[k, at, :], (8, LANES))
                    match = half == sub_iota
                    a_hi = jnp.where(match, jnp.broadcast_to(hi_s[k, at, :], (8, LANES)), 0.0)
                    a_lo = jnp.where(match, jnp.broadcast_to(lo_s[k, at, :], (8, LANES)), 0.0)
                    a = jnp.concatenate([a_hi, a_lo], axis=0).astype(jnp.bfloat16)
                    left.append(jnp.concatenate([a, pad] if t == 0 else [pad, a], axis=0))
                    lane = jnp.broadcast_to(lane_s[k, at, :], (HALF, LANES)).astype(jnp.bfloat16)
                    right.append(jnp.where(lane == half_iota, one, nil))
            product = lax.dot_general(
                jnp.concatenate(left, axis=1),
                jnp.concatenate(right, axis=1),
                (((1,), (1,)), ((), ())),
                preferred_element_type=jnp.float32,
            )
            for t in range(2):
                total = product[16 * t : 16 * t + 8] + product[16 * t + 8 : 16 * t + 16]
                sums_s[pl.ds(pl.multiple_of(8 * (t0 + 2 * pair + t), 8), 8), 0:HALF] = total
                out.append(total)
        return tuple(
            acc + sum(out[t] for t in range(8) if t % blocks == b)
            for b, acc in enumerate(remote_sums)
        )

    start = tuple(jnp.zeros((8, HALF), jnp.float32) for _ in range(blocks))
    remote_sums = lax.fori_loop(0, tiles // 8, eight_tiles, start, unroll=UNROLL[2])
    for b in range(blocks):
        for i in range(2):
            both = jnp.concatenate([remote_sums[b][4 + 2 * i : 5 + 2 * i], remote_sums[b][5 + 2 * i : 6 + 2 * i]], axis=1)
            remote_out[2 * b + i : 2 * b + i + 1, :] = both
    up_out[...] = remote_out[base + 3 : base + 4, :]
    down_out[...] = remote_out[base + 1 : base + 2, :]
    near_out[0:1, :] = read(remote_out, base + 2 - 2 * odd)
    near_out[1:2, :] = read(remote_out, base + 2 * odd)
    for i in range(group):
        owner = me ^ i
        if per_row == 1:
            row = read(remote_out, owner)
        else:
            row = read(remote_out, owner // per_row)
            row = pltpu.roll(jnp.broadcast_to(row, (8, LANES)), (LANES - (owner % per_row) * group_size) % LANES, 1)[0:1, :group_size]
        if i == 0:
            group_keep[...] = row
        else:
            bit = i.bit_length() - 1
            group_outs[bit][i - (1 << bit) : i - (1 << bit) + 1, :] = row
    sums_s[8 * tiles : 8 * tiles + 32, :] = jnp.zeros((32, LANES), jnp.float32)
    for a in range(rows // 8):
        parts = []
        for odd in range(2):
            total = jnp.zeros((8, LANES), jnp.float32)
            for i in range(4):
                lowest = 16 * a + odd + 2 - i
                if lowest >= 0:
                    got = sums_s[pl.ds(8 * lowest + i, 8, stride=16), :]
                else:
                    got = sums_s[pl.ds(8 * (lowest + 2) + i, 8, stride=16), :]
                    got = jnp.where(sub_iota == 0, 0.0, pltpu.roll(got, 1, 0))
                total = total + got
            parts.append(total)
        own_out[8 * a : 8 * a + 8, :] = jnp.where(lane_iota < HALF, parts[0], pltpu.roll(parts[1], HALF, 1))


def faces_call(prepared, rows, group, group_size, received):
    tiles = prepared[0].shape[1]
    bits = group.bit_length() - 1
    blocks = (group * group_size + 4 * LANES) // (2 * LANES)
    f32 = jnp.float32
    group_rows = [1] + [1 << bit for bit in range(bits)]
    return pl.pallas_call(
        lambda *refs: faces_kernel(tiles, blocks, group, *refs),
        out_shape=(
            jax.ShapeDtypeStruct((rows, LANES), f32),
            *[jax.ShapeDtypeStruct((n, group_size), f32) for n in group_rows],
            jax.ShapeDtypeStruct((2, LANES), f32),
            jax.ShapeDtypeStruct((1, LANES), f32),
            jax.ShapeDtypeStruct((1, LANES), f32),
        ),
        in_specs=[VMEM] * (len(prepared) + len(received)),
        out_specs=(VMEM,) * (bits + 5),
        scratch_shapes=[
            pltpu.VMEM((3, tiles, LANES), f32),
            pltpu.VMEM((3, tiles, LANES), f32),
            pltpu.VMEM((8 * tiles + 128, LANES), f32),
            pltpu.VMEM((2 * blocks, LANES), f32),
            pltpu.VMEM((2 * blocks, LANES), f32),
        ],
        cost_estimate=pl.CostEstimate(flops=COST[1], bytes_accessed=1 << 20, transcendentals=0),
        compiler_params=pltpu.CompilerParams(vmem_limit_bytes=6 * 2**20),
        name="faces",
    )(*prepared, *received)


def scatter_kernel(rows, bits, own_ref, sub_ref, pat_ref, direct_ref, up_ref, down_ref, *refs):
    out_ref = refs[-1]
    row_iota = iota((rows, LANES), 0)
    lane_iota = iota((LANES, LANES), 0)
    odd = jnp.broadcast_to(lax.axis_index("patch") & 1, (1, LANES)) == 1
    direct = direct_ref[0:1, :]
    group_back = refs[0][...]
    for i in range(bits):
        ref = refs[i + 1]
        for at in range(0, ref.shape[0], 1 << (bits - 1 - i)):
            group_back = group_back + ref[at : at + 1, :]
    backs = [
        group_back,
        jnp.where(odd, down_ref[1:2, :], direct),
        down_ref[0:1, :],
        jnp.where(odd, direct, up_ref[1:2, :]),
        up_ref[0:1, :],
    ]
    left, right = [], []
    for j in range(5):
        index = sub_ref[0:1, :] if j == 0 else pat_ref[j - 1 : j, :]
        value = backs[j]
        width = index.shape[1]
        hi = value.astype(jnp.bfloat16).astype(jnp.float32)
        match = jnp.broadcast_to(index >> 7, (rows, width)) == row_iota[:, :width]
        a_hi = jnp.where(match, jnp.broadcast_to(hi, (rows, width)), 0.0)
        a_lo = jnp.where(match, jnp.broadcast_to(value - hi, (rows, width)), 0.0)
        left.append(jnp.concatenate([a_hi, a_lo], axis=0).astype(jnp.bfloat16))
        spot = jnp.broadcast_to(index & (LANES - 1), (LANES, width)) == lane_iota[:, :width]
        right.append(jnp.where(spot, 1.0, 0.0).astype(jnp.bfloat16))
    product = 0.0
    for part in ([0], [1, 2, 3, 4]) if left[0].shape[1] < LANES else ([0, 1, 2, 3, 4],):
        product = product + lax.dot_general(
            jnp.concatenate([left[j] for j in part], axis=1),
            jnp.concatenate([right[j] for j in part], axis=1),
            (((1,), (1,)), ((), ())),
            preferred_element_type=jnp.float32,
        )
    out_ref[...] = own_ref[...] + product[:rows] + product[rows:]


def in_hbm(*arrays):
    return [pltpu.with_memory_space_constraint(array, pltpu.HBM) for array in arrays]


def stack(parts):
    return parts[0] if len(parts) == 1 else jnp.concatenate(parts, axis=0)


def per_device(heat, basis, area, corners, send_sub, send_pat, live_faces):
    owned = heat.shape[0]
    rows = owned // LANES
    group = lax.axis_size("sub")
    group_size = send_sub.shape[0]
    block_size = send_pat.shape[1]
    offsets = send_pat.shape[0]
    remote_len = group * group_size + offsets * block_size
    assert offsets == 4 and block_size == LANES and LANES % group_size == 0
    assert group & (group - 1) == 0 and remote_len in (512, 1024, 2048)
    assert lax.axis_size("patch") % 2 == 0
    bits = group.bit_length() - 1
    f32 = jnp.float32
    heat2 = heat.reshape(rows, LANES)
    sub2 = send_sub.reshape(1, group_size)

    mine, near, up, down, sub_index, pat_index = pl.pallas_call(
        lambda *refs: send_kernel(rows, *refs),
        out_shape=(
            jax.ShapeDtypeStruct((1, group_size), f32),
            jax.ShapeDtypeStruct((2, LANES), f32),
            jax.ShapeDtypeStruct((1, LANES), f32),
            jax.ShapeDtypeStruct((1, LANES), f32),
            jax.ShapeDtypeStruct(sub2.shape, jnp.int32),
            jax.ShapeDtypeStruct(send_pat.shape, jnp.int32),
        ),
        in_specs=[HBM] * 3,
        out_specs=(VMEM,) * 6,
        scratch_shapes=[
            pltpu.VMEM(heat2.shape, f32),
            pltpu.SemaphoreType.DMA((3,)),
        ],
        compiler_params=pltpu.CompilerParams(vmem_limit_bytes=2 * 2**20),
        name="send_gather",
    )(*in_hbm(heat2, sub2, send_pat))
    prepared = prepare_call(live_faces, heat2, corners, basis, area, remote_len // (2 * LANES))
    direct = swap(near, "patch", 1)
    relay = direct[1:2]
    from_below = shift(jnp.concatenate([up, relay]), "patch", 2)
    from_above = shift(jnp.concatenate([down, relay]), "patch", -2)
    held = [mine]
    for bit in range(bits):
        held.append(swap(stack(held), "sub", 1 << bit))

    own_sums, keep, *outs, near, up, down = faces_call(
        prepared, rows, group, group_size, (direct, from_below, from_above, *held)
    )

    direct = swap(near, "patch", 1)
    relay = direct[1:2]
    from_above = shift(jnp.concatenate([down, relay]), "patch", -2)
    from_below = shift(jnp.concatenate([up, relay]), "patch", 2)
    pieces, group_back = [], []
    for bit in reversed(range(bits)):
        width = 1 << bit
        got = swap(stack([outs[bit]] + [p[width : 2 * width] for p in pieces]), "sub", width)
        group_back.append(got)
        pieces = [p[:width] for p in pieces] + [
            got[at : at + width] for at in range(0, got.shape[0], width)
        ]

    result = pl.pallas_call(
        lambda *refs: scatter_kernel(rows, bits, *refs),
        out_shape=jax.ShapeDtypeStruct((rows, LANES), f32),
        in_specs=[VMEM] * (7 + bits),
        out_specs=VMEM,
        compiler_params=pltpu.CompilerParams(vmem_limit_bytes=4 * 2**20),
        name="scatter_back",
    )(own_sums, sub_index, pat_index, direct, from_below, from_above, keep, *group_back)
    return result.reshape(-1)


def solution(mesh):
    placed = (
        P(("patch", "sub")),
        P(None, ("patch", "sub")),
        P(("patch", "sub")),
        P(None, ("patch", "sub")),
        P(("patch", "sub")),
        P(None, ("patch", "sub")),
        P(("patch", "sub")),
    )

    return jax.shard_map(per_device, mesh=mesh, in_specs=placed, out_specs=P(("patch", "sub")), check_vma=False)
```

```python
import jax
import jax.numpy as jnp
from jax import lax
from jax.experimental import pallas as pl
from jax.experimental.pallas import tpu as pltpu
from jax.sharding import PartitionSpec as P


LANES = 128
HALF = 64
QUARTER = 32
UNROLL = (16, 16, 16)
COST = (1 << 24, 1 << 24)
VMEM = pl.BlockSpec(memory_space=pltpu.VMEM)
HBM = pl.BlockSpec(memory_space=pltpu.HBM)
SMEM = pl.BlockSpec(memory_space=pltpu.SMEM)


def swap_far(x, axis, outer):
    n = lax.axis_size(axis)
    low = [i for i in range(n) if (i % 4 >= 2) == outer]
    return lax.ppermute(x, axis, [(i, (i + 2) % n) for i in low] + [((i + 2) % n, i) for i in low])


def swap(x, axis, bit):
    n = lax.axis_size(axis)
    return lax.ppermute(x, axis, [(i, i ^ bit) for i in range(n)])


def iota(shape, dim, dtype=jnp.int32):
    return lax.broadcasted_iota(jnp.int32, shape, dim).astype(dtype)


def lane_gather(table, lanes):
    return jnp.take_along_axis(table, lanes, axis=1, mode="promise_in_bounds")


def read(ref, at):
    return ref[pl.ds(at, 1), :]


def send_kernel(
    rows, heat_hbm, sub_hbm, pat_hbm, group_ref, near_ref, outer_ref, inner_ref, sub_ref, pat_ref, heat_ref, sems
):
    copies = [
        pltpu.make_async_copy(source, target, sems.at[i])
        for i, (source, target) in enumerate(((heat_hbm, heat_ref), (sub_hbm, sub_ref), (pat_hbm, pat_ref)))
    ]
    for copy in copies:
        copy.start()
    for copy in copies:
        copy.wait()
    blocks = rows // 8
    sub_iota = iota((8, LANES), 0)
    odd = lax.axis_index("patch") & 1
    high = (lax.axis_index("patch") >> 1) & 1
    for j in range(5):
        if j == 0:
            index = sub_ref[0:1, :]
        else:
            index = read(pat_ref, (3 - 2 * high, 1 + 2 * high, 2 * odd, 2 - 2 * odd)[j - 1])
        index = jnp.broadcast_to(index, (8, index.shape[1]))
        if index.shape[1] < LANES:
            index = jnp.concatenate([index] * (LANES // index.shape[1]), axis=1)
        lane = index & (LANES - 1)
        row = index >> 7
        total = jnp.zeros((8, LANES), jnp.float32)
        for a in range(blocks):
            got = lane_gather(heat_ref[8 * a : 8 * a + 8, :], lane)
            total = jnp.where(row == sub_iota + 8 * a, got, total)
        total = jnp.where((row & 7) == sub_iota, total, 0.0)
        total = jnp.sum(total, axis=0, keepdims=True)
        if j == 0:
            group_ref[...] = total[:, : sub_ref.shape[1]]
        elif j < 3:
            (outer_ref, inner_ref)[j - 1][...] = total
        else:
            near_ref[j - 3 : j - 2, :] = total


def by_side(high, outer_ref, inner_ref):
    is_high = jnp.broadcast_to(high, outer_ref.shape) == 1
    outer, inner = outer_ref[...], inner_ref[...]
    return jnp.where(is_high, inner, outer), jnp.where(is_high, outer, inner)


def prepare_kernel(
    owned,
    tiles,
    blocks,
    live_ref,
    heat_hbm,
    corner_hbm,
    basis_hbm,
    area_hbm,
    near_out,
    off_out,
    part_out,
    lane_out,
    basis_out,
    last_out,
    weight_out,
    heat_ref,
    corner_ref,
    basis_ref,
    win,
    corner_s,
    sems,
):
    copies = [
        pltpu.make_async_copy(source, target, sems.at[i])
        for i, (source, target) in enumerate(
            ((corner_hbm, corner_ref), (heat_hbm, heat_ref), (basis_hbm, basis_ref), (area_hbm, weight_out))
        )
    ]
    for copy in copies:
        copy.start()
    rows = owned // LANES
    lane_iota = iota((8, LANES), 1)
    sub_iota = iota((8, LANES), 0)
    copies[1].wait()
    zero = jnp.zeros((8, LANES), jnp.float32)
    win[0:8, :] = zero
    win[2 * rows : 2 * rows + 8, :] = zero
    for a in range(rows // 8):
        here = heat_ref[8 * a : 8 * a + 8, :]
        if a + 1 < rows // 8:
            after = heat_ref[8 * a + 1 : 8 * a + 9, :]
        else:
            after = jnp.concatenate([heat_ref[8 * a + 1 : 8 * a + 8, :], zero[0:1]], axis=0)
        both = jnp.where(lane_iota < HALF, after, here)
        win[pl.ds(16 * a + 2, 8, stride=2), :] = here
        win[pl.ds(16 * a + 3, 8, stride=2), :] = pltpu.roll(both, HALF, 1)
    first = pltpu.roll(jnp.broadcast_to(heat_ref[0:1, :], (8, LANES)), HALF, 1)
    win[1:2, :] = jnp.where(lane_iota < HALF, 0.0, first)[0:1]
    copies[0].wait()

    def spread_corners(t, carry):
        at = pl.ds(pl.multiple_of(LANES * t, LANES), LANES)
        corner_s[pl.ds(pl.multiple_of(4 * t, 4), 3), :] = corner_ref[:, at]
        return carry

    lax.fori_loop(0, tiles, spread_corners, 0, unroll=UNROLL[0])

    def near_values(g, carry):
        t0 = pl.multiple_of(8 * g, 8)
        tile = t0 + sub_iota
        near = [win[pl.ds(t0, 8), :], win[pl.ds(t0 + 2, 8), :]]
        near_start = HALF * tile - LANES
        far_start = owned + 2 * LANES * (sub_iota % blocks) - 2 * LANES
        at = pl.ds(t0, 8)
        for k in range(3):
            pos = corner_s[pl.ds(4 * t0 + k, 8, stride=4), :]
            off = pos - jnp.where(pos >= owned, far_start, near_start)
            lane = off & (LANES - 1)
            near_out[k, at, :] = jnp.where(
                off >= LANES, lane_gather(near[1], lane), lane_gather(near[0], lane)
            )
            off_out[k, at, :] = off
            part_out[k, at, :] = (off >> 5).astype(jnp.float32)
            lane_out[k, at, :] = (off & (QUARTER - 1)).astype(jnp.float32)
        return carry

    lax.fori_loop(0, tiles // 8, near_values, 0, unroll=UNROLL[1])
    copies[2].wait()

    def spread_basis(t, carry):
        at = pl.ds(pl.multiple_of(LANES * t, LANES), LANES)
        nine = basis_ref[:, at].astype(jnp.float32)
        basis_out[pl.ds(pl.multiple_of(8 * t, 8), 8), :] = nine[0:8]
        last_out[pl.ds(t, 1), :] = nine[8:9]
        return carry

    lax.fori_loop(0, tiles, spread_basis, 0, unroll=UNROLL[0])
    copies[3].wait()
    live = live_ref[0]
    for t0 in range(0, tiles, 8):
        slot = (t0 + sub_iota) * LANES + lane_iota
        weight_out[t0 : t0 + 8, :] = jnp.where(slot < live, -weight_out[t0 : t0 + 8, :], 0.0)


def prepare_call(live_faces, heat2, corners, basis, area, blocks):
    rows = heat2.shape[0]
    tiles = corners.shape[1] // LANES
    f32 = jnp.float32
    per_corner = (3, tiles, LANES)
    return pl.pallas_call(
        lambda *refs: prepare_kernel(rows * LANES, tiles, blocks, *refs),
        out_shape=(
            jax.ShapeDtypeStruct(per_corner, f32),
            jax.ShapeDtypeStruct(per_corner, jnp.int32),
            jax.ShapeDtypeStruct(per_corner, f32),
            jax.ShapeDtypeStruct(per_corner, f32),
            jax.ShapeDtypeStruct((8 * tiles, LANES), f32),
            jax.ShapeDtypeStruct((tiles, LANES), f32),
            jax.ShapeDtypeStruct((tiles, LANES), f32),
        ),
        in_specs=[SMEM] + [HBM] * 4,
        out_specs=(VMEM,) * 7,
        scratch_shapes=[
            pltpu.VMEM(heat2.shape, f32),
            pltpu.VMEM(corners.shape, jnp.int32),
            pltpu.VMEM(basis.shape, basis.dtype),
            pltpu.VMEM((2 * rows + 8, LANES), f32),
            pltpu.VMEM((4 * tiles, LANES), jnp.int32),
            pltpu.SemaphoreType.DMA((4,)),
        ],
        cost_estimate=pl.CostEstimate(flops=COST[0], bytes_accessed=1 << 20, transcendentals=0),
        compiler_params=pltpu.CompilerParams(vmem_limit_bytes=6 * 2**20),
        name="prepare",
    )(live_faces, *in_hbm(heat2, corners, basis, area.reshape(tiles, LANES)))


def faces_kernel(tiles, blocks, group, *refs):
    near_ref, off_ref, part_s, lane_s, basis_s, last_s, weight_ref, direct_ref, outer_ref, inner_ref, *refs = refs
    bits = group.bit_length() - 1
    group_refs = refs[: bits + 1]
    own_out, group_keep, *group_outs, near_out, outer_out, inner_out = refs[bits + 1 : 2 * bits + 6]
    hi_s, lo_s, sums_s, remote_ref, remote_out = refs[2 * bits + 6 :]
    group_size = group_keep.shape[1]
    odd = lax.axis_index("patch") & 1
    me = lax.axis_index("sub")
    rows = own_out.shape[0]
    lane_iota = iota((8, LANES), 1)
    sub_iota = iota((8, LANES), 0)
    per_row = LANES // group_size
    for q in range(group // per_row):
        parts = []
        for e in range(per_row):
            from_me = me ^ (q * per_row + e)
            part = group_refs[0][...]
            for bit in range(bits):
                got = read(group_refs[bit + 1], from_me & ((1 << bit) - 1))
                part = jnp.where(from_me >> bit == 1, got, part)
            parts.append(part)
        remote_ref[q : q + 1, :] = parts[0] if per_row == 1 else jnp.concatenate(parts, axis=1)
    base = group // per_row
    is_odd = jnp.broadcast_to(odd, (1, LANES)) == 1
    direct = direct_ref[0:1, :]
    high = (lax.axis_index("patch") >> 1) & 1
    below, above = by_side(high, outer_ref, inner_ref)
    remote_ref[base : base + 1, :] = jnp.where(is_odd, direct, below[1:2])
    remote_ref[base + 1 : base + 2, :] = below[0:1]
    remote_ref[base + 2 : base + 3, :] = jnp.where(is_odd, above[1:2], direct)
    remote_ref[base + 3 : base + 4, :] = above[0:1]
    remote_rows = [
        jnp.concatenate([remote_ref[2 * (t % blocks) + i : 2 * (t % blocks) + i + 1, :] for t in range(8)], axis=0)
        for i in range(2)
    ]
    lane_row = iota((QUARTER, LANES), 0, jnp.float32).astype(jnp.bfloat16)
    part_row = iota((16, LANES), 0, jnp.float32).astype(jnp.bfloat16)
    one = jnp.ones((QUARTER, LANES), jnp.bfloat16)
    nil = jnp.zeros((QUARTER, LANES), jnp.bfloat16)

    def face_values(g, carry):
        t0 = pl.multiple_of(8 * g, 8)
        at = pl.ds(t0, 8)
        values = []
        for k in range(3):
            off = off_ref[k, at, :]
            lane = off & (LANES - 1)
            far = jnp.where(
                off >= 3 * LANES, lane_gather(remote_rows[1], lane), lane_gather(remote_rows[0], lane)
            )
            values.append(jnp.where(off >= 2 * LANES, far, near_ref[k, at, :]))
        basis = [basis_s[pl.ds(8 * t0 + i, 8, stride=8), :] for i in range(8)] + [last_s[at, :]]
        grad = [sum(basis[3 * k + c] * values[k] for k in range(3)) for c in range(3)]
        square = grad[0] * grad[0] + grad[1] * grad[1] + grad[2] * grad[2]
        scale = weight_ref[at, :] / jnp.maximum(jnp.sqrt(square), 1.0)
        field = [grad[c] * scale for c in range(3)]
        for k in range(3):
            term = sum(basis[3 * k + c] * field[c] for c in range(3))
            hi = term.astype(jnp.bfloat16).astype(jnp.float32)
            hi_s[k, at, :] = hi
            lo_s[k, at, :] = term - hi
        return carry

    lax.fori_loop(0, tiles // 8, face_values, 0, unroll=UNROLL[1])

    def spread_row(ref, k, t, rows):
        return jnp.broadcast_to(ref[k, pl.ds(t, 1), :], (rows, LANES)).astype(jnp.bfloat16)

    def tile_sums(t):
        left, right = [], []
        for k in range(3):
            match = spread_row(part_s, k, t, 16) == part_row
            a_hi = jnp.where(match, spread_row(hi_s, k, t, 16), nil[:16])
            a_lo = jnp.where(match, spread_row(lo_s, k, t, 16), nil[:16])
            left.append(jnp.concatenate([a_hi, a_lo], axis=0))
            right.append(jnp.where(spread_row(lane_s, k, t, QUARTER) == lane_row, one, nil))
        product = lax.dot_general(
            jnp.concatenate(left, axis=1),
            jnp.concatenate(right, axis=1),
            (((1,), (1,)), ((), ())),
            preferred_element_type=jnp.float32,
        )
        return product[:16] + product[16:]

    def eight_tiles(g, remote_sums):
        remote_sums = list(remote_sums)
        for i in range(8):
            t = 8 * g + i
            total = tile_sums(t)
            sums_s[pl.ds(pl.multiple_of(8 * t + 8, 8), 8), 0:QUARTER] = total[:8]
            remote_sums[i % blocks] = remote_sums[i % blocks] + total[8:]
        return tuple(remote_sums)

    start = tuple(jnp.zeros((8, QUARTER), jnp.float32) for _ in range(blocks))
    remote_sums = lax.fori_loop(0, tiles // 8, eight_tiles, start, unroll=UNROLL[2])
    for b in range(blocks):
        for i in range(2):
            row = [remote_sums[b][4 * i + e : 4 * i + e + 1] for e in range(4)]
            remote_out[2 * b + i : 2 * b + i + 1, :] = jnp.concatenate(row, axis=1)
    outer_out[...] = read(remote_out, base + 1 + 2 * high)
    inner_out[...] = read(remote_out, base + 3 - 2 * high)
    near_out[0:1, :] = read(remote_out, base + 2 - 2 * odd)
    near_out[1:2, :] = read(remote_out, base + 2 * odd)
    for i in range(group):
        owner = me ^ i
        if per_row == 1:
            row = read(remote_out, owner)
        else:
            row = read(remote_out, owner // per_row)
            row = pltpu.roll(jnp.broadcast_to(row, (8, LANES)), (LANES - (owner % per_row) * group_size) % LANES, 1)[0:1, :group_size]
        if i == 0:
            group_keep[...] = row
        else:
            bit = i.bit_length() - 1
            group_outs[bit][i - (1 << bit) : i - (1 << bit) + 1, :] = row
    sums_s[0:8, :] = jnp.zeros((8, LANES), jnp.float32)
    sums_s[8 * tiles + 8 : 8 * tiles + 32, :] = jnp.zeros((24, LANES), jnp.float32)
    for a in range(rows // 8):
        whole = None
        for e in range(4):
            total = None
            for h in range(e & 1, 8, 2):
                tile = 16 * a + (e + 4 - h) // 2
                got = sums_s[pl.ds(8 * (tile + 1) + h, 8, stride=16), :]
                total = got if total is None else total + got
            if e == 0:
                whole = total
            else:
                whole = jnp.where(lane_iota >= QUARTER * e, pltpu.roll(total, QUARTER * e, 1), whole)
        own_out[8 * a : 8 * a + 8, :] = whole


def faces_call(prepared, rows, group, group_size, received):
    tiles = prepared[0].shape[1]
    bits = group.bit_length() - 1
    blocks = (group * group_size + 4 * LANES) // (2 * LANES)
    f32 = jnp.float32
    group_rows = [1] + [1 << bit for bit in range(bits)]
    return pl.pallas_call(
        lambda *refs: faces_kernel(tiles, blocks, group, *refs),
        out_shape=(
            jax.ShapeDtypeStruct((rows, LANES), f32),
            *[jax.ShapeDtypeStruct((n, group_size), f32) for n in group_rows],
            jax.ShapeDtypeStruct((2, LANES), f32),
            jax.ShapeDtypeStruct((1, LANES), f32),
            jax.ShapeDtypeStruct((1, LANES), f32),
        ),
        in_specs=[VMEM] * (len(prepared) + len(received)),
        out_specs=(VMEM,) * (bits + 5),
        scratch_shapes=[
            pltpu.VMEM((3, tiles, LANES), f32),
            pltpu.VMEM((3, tiles, LANES), f32),
            pltpu.VMEM((8 * tiles + 128, LANES), f32),
            pltpu.VMEM((2 * blocks, LANES), f32),
            pltpu.VMEM((2 * blocks, LANES), f32),
        ],
        cost_estimate=pl.CostEstimate(flops=COST[1], bytes_accessed=1 << 20, transcendentals=0),
        compiler_params=pltpu.CompilerParams(vmem_limit_bytes=6 * 2**20),
        name="faces",
    )(*prepared, *received)


def scatter_kernel(rows, bits, own_ref, sub_ref, pat_ref, direct_ref, outer_ref, inner_ref, *refs):
    out_ref = refs[-1]
    row_iota = iota((rows, LANES), 0)
    lane_iota = iota((LANES, LANES), 0)
    odd = jnp.broadcast_to(lax.axis_index("patch") & 1, (1, LANES)) == 1
    direct = direct_ref[0:1, :]
    below, above = by_side((lax.axis_index("patch") >> 1) & 1, outer_ref, inner_ref)
    group_back = refs[0][...]
    for i in range(bits):
        ref = refs[i + 1]
        for at in range(0, ref.shape[0], 1 << (bits - 1 - i)):
            group_back = group_back + ref[at : at + 1, :]
    backs = [
        group_back,
        jnp.where(odd, above[1:2], direct),
        above[0:1],
        jnp.where(odd, direct, below[1:2]),
        below[0:1],
    ]
    left, right = [], []
    for j in range(5):
        index = sub_ref[0:1, :] if j == 0 else pat_ref[j - 1 : j, :]
        value = backs[j]
        width = index.shape[1]
        hi = value.astype(jnp.bfloat16).astype(jnp.float32)
        match = jnp.broadcast_to(index >> 7, (rows, width)) == row_iota[:, :width]
        a_hi = jnp.where(match, jnp.broadcast_to(hi, (rows, width)), 0.0)
        a_lo = jnp.where(match, jnp.broadcast_to(value - hi, (rows, width)), 0.0)
        left.append(jnp.concatenate([a_hi, a_lo], axis=0).astype(jnp.bfloat16))
        spot = jnp.broadcast_to(index & (LANES - 1), (LANES, width)) == lane_iota[:, :width]
        right.append(jnp.where(spot, 1.0, 0.0).astype(jnp.bfloat16))
    product = 0.0
    for part in ([0], [1, 2, 3, 4]) if left[0].shape[1] < LANES else ([0, 1, 2, 3, 4],):
        product = product + lax.dot_general(
            jnp.concatenate([left[j] for j in part], axis=1),
            jnp.concatenate([right[j] for j in part], axis=1),
            (((1,), (1,)), ((), ())),
            preferred_element_type=jnp.float32,
        )
    out_ref[...] = own_ref[...] + product[:rows] + product[rows:]


def in_hbm(*arrays):
    return [pltpu.with_memory_space_constraint(array, pltpu.HBM) for array in arrays]


def stack(parts):
    return parts[0] if len(parts) == 1 else jnp.concatenate(parts, axis=0)


def per_device(heat, basis, area, corners, send_sub, send_pat, live_faces):
    owned = heat.shape[0]
    rows = owned // LANES
    group = lax.axis_size("sub")
    group_size = send_sub.shape[0]
    block_size = send_pat.shape[1]
    offsets = send_pat.shape[0]
    remote_len = group * group_size + offsets * block_size
    assert offsets == 4 and block_size == LANES and LANES % group_size == 0
    assert group & (group - 1) == 0 and remote_len in (512, 1024, 2048)
    assert lax.axis_size("patch") % 4 == 0
    bits = group.bit_length() - 1
    f32 = jnp.float32
    heat2 = heat.reshape(rows, LANES)
    sub2 = send_sub.reshape(1, group_size)

    mine, near, outer, inner, sub_index, pat_index = pl.pallas_call(
        lambda *refs: send_kernel(rows, *refs),
        out_shape=(
            jax.ShapeDtypeStruct((1, group_size), f32),
            jax.ShapeDtypeStruct((2, LANES), f32),
            jax.ShapeDtypeStruct((1, LANES), f32),
            jax.ShapeDtypeStruct((1, LANES), f32),
            jax.ShapeDtypeStruct(sub2.shape, jnp.int32),
            jax.ShapeDtypeStruct(send_pat.shape, jnp.int32),
        ),
        in_specs=[HBM] * 3,
        out_specs=(VMEM,) * 6,
        scratch_shapes=[
            pltpu.VMEM(heat2.shape, f32),
            pltpu.SemaphoreType.DMA((3,)),
        ],
        compiler_params=pltpu.CompilerParams(vmem_limit_bytes=2 * 2**20),
        name="send_gather",
    )(*in_hbm(heat2, sub2, send_pat))
    prepared = prepare_call(live_faces, heat2, corners, basis, area, remote_len // (2 * LANES))
    direct = swap(near, "patch", 1)
    relay = direct[1:2]
    outer = swap_far(jnp.concatenate([outer, relay]), "patch", True)
    inner = swap_far(jnp.concatenate([inner, relay]), "patch", False)
    held = [mine]
    for bit in range(bits):
        held.append(swap(stack(held), "sub", 1 << bit))

    own_sums, keep, *outs, near, outer, inner = faces_call(
        prepared, rows, group, group_size, (direct, outer, inner, *held)
    )

    direct = swap(near, "patch", 1)
    relay = direct[1:2]
    outer = swap_far(jnp.concatenate([outer, relay]), "patch", True)
    inner = swap_far(jnp.concatenate([inner, relay]), "patch", False)
    pieces, group_back = [], []
    for bit in reversed(range(bits)):
        width = 1 << bit
        got = swap(stack([outs[bit]] + [p[width : 2 * width] for p in pieces]), "sub", width)
        group_back.append(got)
        pieces = [p[:width] for p in pieces] + [
            got[at : at + width] for at in range(0, got.shape[0], width)
        ]

    result = pl.pallas_call(
        lambda *refs: scatter_kernel(rows, bits, *refs),
        out_shape=jax.ShapeDtypeStruct((rows, LANES), f32),
        in_specs=[VMEM] * (7 + bits),
        out_specs=VMEM,
        compiler_params=pltpu.CompilerParams(vmem_limit_bytes=4 * 2**20),
        name="scatter_back",
    )(own_sums, sub_index, pat_index, direct, outer, inner, keep, *group_back)
    return result.reshape(-1)


def solution(mesh):
    placed = (
        P(("patch", "sub")),
        P(None, ("patch", "sub")),
        P(("patch", "sub")),
        P(None, ("patch", "sub")),
        P(("patch", "sub")),
        P(None, ("patch", "sub")),
        P(("patch", "sub")),
    )

    return jax.shard_map(per_device, mesh=mesh, in_specs=placed, out_specs=P(("patch", "sub")), check_vma=False)
```

```python
import jax
import jax.numpy as jnp
from jax import lax
from jax.experimental import pallas as pl
from jax.experimental.pallas import tpu as pltpu
from jax.sharding import PartitionSpec as P


LANES = 128
HALF = 64
QUARTER = 32
COST = (1 << 24, 1 << 24)
VMEM = pl.BlockSpec(memory_space=pltpu.VMEM)
HBM = pl.BlockSpec(memory_space=pltpu.HBM)
SMEM = pl.BlockSpec(memory_space=pltpu.SMEM)


def swap_far(x, axis, outer):
    n = lax.axis_size(axis)
    low = [i for i in range(n) if (i % 4 >= 2) == outer]
    return lax.ppermute(x, axis, [(i, (i + 2) % n) for i in low] + [((i + 2) % n, i) for i in low])


def swap(x, axis, bit):
    n = lax.axis_size(axis)
    return lax.ppermute(x, axis, [(i, i ^ bit) for i in range(n)])


def iota(shape, dim, dtype=jnp.int32):
    return lax.broadcasted_iota(jnp.int32, shape, dim).astype(dtype)


def lane_gather(table, lanes):
    return jnp.take_along_axis(table, lanes, axis=1, mode="promise_in_bounds")


def read(ref, at):
    return ref[pl.ds(at, 1), :]


def send_kernel(
    rows, heat_hbm, sub_hbm, pat_hbm, group_ref, near_ref, outer_ref, inner_ref, sub_ref, pat_ref, heat_ref, sems
):
    copies = [
        pltpu.make_async_copy(source, target, sems.at[i])
        for i, (source, target) in enumerate(((heat_hbm, heat_ref), (sub_hbm, sub_ref), (pat_hbm, pat_ref)))
    ]
    for copy in copies:
        copy.start()
    for copy in copies:
        copy.wait()
    blocks = rows // 8
    sub_iota = iota((8, LANES), 0)
    odd = lax.axis_index("patch") & 1
    high = (lax.axis_index("patch") >> 1) & 1
    for j in range(5):
        if j == 0:
            index = sub_ref[0:1, :]
        else:
            index = read(pat_ref, (3 - 2 * high, 1 + 2 * high, 2 * odd, 2 - 2 * odd)[j - 1])
        index = jnp.broadcast_to(index, (8, index.shape[1]))
        if index.shape[1] < LANES:
            index = jnp.concatenate([index] * (LANES // index.shape[1]), axis=1)
        lane = index & (LANES - 1)
        row = index >> 7
        total = jnp.zeros((8, LANES), jnp.float32)
        for a in range(blocks):
            got = lane_gather(heat_ref[8 * a : 8 * a + 8, :], lane)
            total = jnp.where(row == sub_iota + 8 * a, got, total)
        total = jnp.where((row & 7) == sub_iota, total, 0.0)
        total = jnp.sum(total, axis=0, keepdims=True)
        if j == 0:
            group_ref[...] = total[:, : sub_ref.shape[1]]
        elif j < 3:
            (outer_ref, inner_ref)[j - 1][0:1, :] = total
        elif j == 3:
            near_ref[...] = total
        else:
            outer_ref[1:2, :] = total
            inner_ref[1:2, :] = total


def by_side(high, outer_ref, inner_ref):
    is_high = jnp.broadcast_to(high, outer_ref.shape) == 1
    outer, inner = outer_ref[...], inner_ref[...]
    return jnp.where(is_high, inner, outer), jnp.where(is_high, outer, inner)


def prepare_kernel(
    owned,
    tiles,
    blocks,
    live_ref,
    heat_hbm,
    corner_hbm,
    basis_hbm,
    area_hbm,
    near_out,
    off_out,
    part_out,
    lane_out,
    basis_out,
    last_out,
    weight_out,
    heat_ref,
    corner_ref,
    basis_ref,
    area_ref,
    win,
    corner_s,
    sems,
):
    copies = [
        pltpu.make_async_copy(source, target, sems.at[i])
        for i, (source, target) in enumerate(
            ((corner_hbm, corner_ref), (heat_hbm, heat_ref), (basis_hbm, basis_ref), (area_hbm, area_ref))
        )
    ]
    for copy in copies:
        copy.start()
    rows = owned // LANES
    lane_iota = iota((8, LANES), 1)
    sub_iota = iota((8, LANES), 0)
    copies[1].wait()
    zero = jnp.zeros((8, LANES), jnp.float32)
    win[0:8, :] = zero
    win[2 * rows : 2 * rows + 8, :] = zero
    for a in range(rows // 8):
        here = heat_ref[8 * a : 8 * a + 8, :]
        if a + 1 < rows // 8:
            after = heat_ref[8 * a + 1 : 8 * a + 9, :]
        else:
            after = jnp.concatenate([heat_ref[8 * a + 1 : 8 * a + 8, :], zero[0:1]], axis=0)
        both = jnp.where(lane_iota < HALF, after, here)
        win[pl.ds(16 * a + 2, 8, stride=2), :] = here
        win[pl.ds(16 * a + 3, 8, stride=2), :] = pltpu.roll(both, HALF, 1)
    first = pltpu.roll(jnp.broadcast_to(heat_ref[0:1, :], (8, LANES)), HALF, 1)
    win[1:2, :] = jnp.where(lane_iota < HALF, 0.0, first)[0:1]
    copies[0].wait()

    per_class = tiles // blocks
    place = [t % blocks * per_class + t // blocks for t in range(tiles)]
    for t in range(tiles):
        corner_s[4 * place[t] : 4 * place[t] + 3, :] = corner_ref[:, LANES * t : LANES * (t + 1)]
    for r in range(blocks):
        for g in range(per_class // 8):
            t0 = 8 * blocks * g + r
            tile = t0 + blocks * sub_iota
            near = [win[pl.ds(t0 + 2 * i, 8, stride=blocks), :] for i in range(2)]
            near_start = HALF * tile - LANES
            far_start = owned + 2 * LANES * r - 2 * LANES
            at = slice(per_class * r + 8 * g, per_class * r + 8 * g + 8)
            for k in range(3):
                pos = corner_s[pl.ds(4 * (per_class * r + 8 * g) + k, 8, stride=4), :]
                off = pos - jnp.where(pos >= owned, far_start, near_start)
                lane = off & (LANES - 1)
                near_out[k, at, :] = jnp.where(
                    off >= LANES, lane_gather(near[1], lane), lane_gather(near[0], lane)
                )
                off_out[k, at, :] = off
                part_out[k, at, :] = (off >> 5).astype(jnp.float32)
                lane_out[k, at, :] = (off & (QUARTER - 1)).astype(jnp.float32)
    copies[2].wait()

    for t in range(tiles):
        nine = basis_ref[:, LANES * t : LANES * (t + 1)].astype(jnp.float32)
        basis_out[8 * place[t] : 8 * place[t] + 8, :] = nine[0:8]
        last_out[place[t] : place[t] + 1, :] = nine[8:9]
    copies[3].wait()
    live = live_ref[0]
    for r in range(blocks):
        for g in range(per_class // 8):
            t0 = 8 * blocks * g + r
            slot = (t0 + blocks * sub_iota) * LANES + lane_iota
            at = slice(per_class * r + 8 * g, per_class * r + 8 * g + 8)
            weight_out[at, :] = jnp.where(slot < live, -area_ref[pl.ds(t0, 8, stride=blocks), :], 0.0)


def prepare_call(live_faces, heat2, corners, basis, area, blocks):
    rows = heat2.shape[0]
    tiles = corners.shape[1] // LANES
    f32 = jnp.float32
    per_corner = (3, tiles, LANES)
    return pl.pallas_call(
        lambda *refs: prepare_kernel(rows * LANES, tiles, blocks, *refs),
        out_shape=(
            jax.ShapeDtypeStruct(per_corner, f32),
            jax.ShapeDtypeStruct(per_corner, jnp.int32),
            jax.ShapeDtypeStruct(per_corner, f32),
            jax.ShapeDtypeStruct(per_corner, f32),
            jax.ShapeDtypeStruct((8 * tiles, LANES), f32),
            jax.ShapeDtypeStruct((tiles, LANES), f32),
            jax.ShapeDtypeStruct((tiles, LANES), f32),
        ),
        in_specs=[SMEM] + [HBM] * 4,
        out_specs=(VMEM,) * 7,
        scratch_shapes=[
            pltpu.VMEM(heat2.shape, f32),
            pltpu.VMEM(corners.shape, jnp.int32),
            pltpu.VMEM(basis.shape, basis.dtype),
            pltpu.VMEM((tiles, LANES), f32),
            pltpu.VMEM((2 * rows + 8, LANES), f32),
            pltpu.VMEM((4 * tiles, LANES), jnp.int32),
            pltpu.SemaphoreType.DMA((4,)),
        ],
        cost_estimate=pl.CostEstimate(flops=COST[0], bytes_accessed=1 << 20, transcendentals=0),
        compiler_params=pltpu.CompilerParams(vmem_limit_bytes=6 * 2**20),
        name="prepare",
    )(live_faces, *in_hbm(heat2, corners, basis, area.reshape(tiles, LANES)))


def class_sums(classes, blocks, prepared, remote_ref, hi_s, lo_s, sums_ref):
    near_ref, off_ref, part_s, lane_s, basis_s, last_s, weight_ref = prepared
    per_class = near_ref.shape[1] // blocks
    lane_row = iota((QUARTER, LANES), 0, jnp.float32).astype(jnp.bfloat16)
    part_row = iota((16, LANES), 0, jnp.float32).astype(jnp.bfloat16)
    one = jnp.ones((QUARTER, LANES), jnp.bfloat16)
    nil = jnp.zeros((QUARTER, LANES), jnp.bfloat16)

    def spread_row(ref, k, row, height):
        return jnp.broadcast_to(ref[k, row : row + 1, :], (height, LANES)).astype(jnp.bfloat16)

    def tile_sums(row):
        left, right = [], []
        for k in range(3):
            match = spread_row(part_s, k, row, 16) == part_row
            a_hi = jnp.where(match, spread_row(hi_s, k, row - per_class * classes[0], 16), nil[:16])
            a_lo = jnp.where(match, spread_row(lo_s, k, row - per_class * classes[0], 16), nil[:16])
            left.append(jnp.concatenate([a_hi, a_lo], axis=0))
            right.append(jnp.where(spread_row(lane_s, k, row, QUARTER) == lane_row, one, nil))
        product = lax.dot_general(
            jnp.concatenate(left, axis=1),
            jnp.concatenate(right, axis=1),
            (((1,), (1,)), ((), ())),
            preferred_element_type=jnp.float32,
        )
        return product[:16] + product[16:]

    for r in classes:
        far_rows = [
            jnp.broadcast_to(remote_ref[2 * (r - classes[0]) + i : 2 * (r - classes[0]) + i + 1, :], (8, LANES))
            for i in range(2)
        ]
        for g in range(per_class // 8):
            row = per_class * r + 8 * g
            at = slice(row, row + 8)
            values = []
            for k in range(3):
                off = off_ref[k, at, :]
                lane = off & (LANES - 1)
                far = jnp.where(
                    off >= 3 * LANES, lane_gather(far_rows[1], lane), lane_gather(far_rows[0], lane)
                )
                values.append(jnp.where(off >= 2 * LANES, far, near_ref[k, at, :]))
            basis = [basis_s[pl.ds(8 * row + i, 8, stride=8), :] for i in range(8)] + [last_s[at, :]]
            grad = [sum(basis[3 * k + c] * values[k] for k in range(3)) for c in range(3)]
            square = grad[0] * grad[0] + grad[1] * grad[1] + grad[2] * grad[2]
            scale = weight_ref[at, :] / jnp.maximum(jnp.sqrt(square), 1.0)
            field = [grad[c] * scale for c in range(3)]
            kept = slice(row - per_class * classes[0], row - per_class * classes[0] + 8)
            for k in range(3):
                term = sum(basis[3 * k + c] * field[c] for c in range(3))
                hi = term.astype(jnp.bfloat16).astype(jnp.float32)
                hi_s[k, kept, :] = hi
                lo_s[k, kept, :] = term - hi
    remote_sums = []
    for r in classes:
        remote_sum = jnp.zeros((8, QUARTER), jnp.float32)
        for i in range(per_class):
            total = tile_sums(per_class * r + i)
            spot = 8 * (blocks * i + r) + 8
            sums_ref[spot : spot + 8, 0:QUARTER] = total[:8]
            remote_sum = remote_sum + total[8:]
        remote_sums.append(remote_sum)
    return remote_sums


def full_rows(quarters):
    return [
        jnp.concatenate([sums[4 * i + e : 4 * i + e + 1] for e in range(4)], axis=1)
        for sums in quarters
        for i in range(2)
    ]


def patch_faces_kernel(classes, blocks, *refs):
    prepared, refs = refs[:7], refs[7:]
    direct_ref, outer_ref, inner_ref, sums_out, near_out, outer_out, inner_out = refs[:7]
    hi_s, lo_s, remote_ref = refs[7:]
    odd = lax.axis_index("patch") & 1
    high = (lax.axis_index("patch") >> 1) & 1
    is_odd = jnp.broadcast_to(odd, (1, LANES)) == 1
    is_high = jnp.broadcast_to(high, (1, LANES)) == 1
    direct = direct_ref[0:1, :]
    below, above = by_side(high, outer_ref, inner_ref)
    relayed = direct_ref[1:2, :]
    remote_ref[0:1, :] = jnp.where(is_odd, direct, relayed)
    remote_ref[1:2, :] = below[0:1]
    remote_ref[2:3, :] = jnp.where(is_odd, relayed, direct)
    remote_ref[3:4, :] = above[0:1]
    rows = full_rows(class_sums(classes, blocks, prepared, remote_ref, hi_s, lo_s, sums_out))
    outer_out[0:1, :] = jnp.where(is_high, rows[3], rows[1])
    inner_out[0:1, :] = jnp.where(is_high, rows[1], rows[3])
    near_out[...] = jnp.where(is_odd, rows[0], rows[2])
    relay = jnp.where(is_odd, rows[2], rows[0])
    outer_out[1:2, :] = relay
    inner_out[1:2, :] = relay


def group_faces_kernel(classes, blocks, group, *refs):
    prepared, sums_ref, refs = refs[:7], refs[7], refs[8:]
    tiles = prepared[0].shape[1]
    bits = group.bit_length() - 1
    group_refs = refs[: bits + 1]
    own_out, group_keep, *group_outs = refs[bits + 1 : 2 * bits + 3]
    hi_s, lo_s, sums_s, remote_ref, remote_out = refs[2 * bits + 3 :]
    group_size = group_keep.shape[1]
    me = lax.axis_index("sub")
    rows = own_out.shape[0]
    lane_iota = iota((8, LANES), 1)
    per_row = LANES // group_size
    for q in range(group // per_row):
        parts = []
        for e in range(per_row):
            from_me = me ^ (q * per_row + e)
            part = group_refs[0][...]
            for bit in range(bits):
                got = read(group_refs[bit + 1], from_me & ((1 << bit) - 1))
                part = jnp.where(from_me >> bit == 1, got, part)
            parts.append(part)
        remote_ref[q : q + 1, :] = parts[0] if per_row == 1 else jnp.concatenate(parts, axis=1)
    for t in range(tiles):
        if t % blocks not in classes:
            sums_s[8 * t + 8 : 8 * t + 16, :] = sums_ref[8 * t + 8 : 8 * t + 16, :]
    sums_s[0:8, :] = jnp.zeros((8, LANES), jnp.float32)
    sums_s[8 * tiles + 8 : 8 * tiles + 32, :] = jnp.zeros((24, LANES), jnp.float32)
    for i, row in enumerate(full_rows(class_sums(classes, blocks, prepared, remote_ref, hi_s, lo_s, sums_s))):
        remote_out[i : i + 1, :] = row
    for i in range(group):
        owner = me ^ i
        row = read(remote_out, owner // per_row)
        if per_row > 1:
            turn = (LANES - (owner % per_row) * group_size) % LANES
            row = pltpu.roll(jnp.broadcast_to(row, (8, LANES)), turn, 1)[0:1, :group_size]
        if i == 0:
            group_keep[...] = row
        else:
            bit = i.bit_length() - 1
            group_outs[bit][i - (1 << bit) : i - (1 << bit) + 1, :] = row
    for a in range(rows // 8):
        whole = None
        for e in range(4):
            total = None
            for h in range(e & 1, 8, 2):
                tile = 16 * a + (e + 4 - h) // 2
                got = sums_s[pl.ds(8 * (tile + 1) + h, 8, stride=16), :]
                total = got if total is None else total + got
            if e == 0:
                whole = total
            else:
                whole = jnp.where(lane_iota >= QUARTER * e, pltpu.roll(total, QUARTER * e, 1), whole)
        own_out[8 * a : 8 * a + 8, :] = whole


def patch_faces_call(prepared, blocks, received):
    tiles = prepared[0].shape[1]
    f32 = jnp.float32
    classes = tuple(range(blocks - 2, blocks))
    kept = (3, 2 * tiles // blocks, LANES)
    return pl.pallas_call(
        lambda *refs: patch_faces_kernel(classes, blocks, *refs),
        out_shape=(
            jax.ShapeDtypeStruct((8 * tiles + 32, LANES), f32),
            jax.ShapeDtypeStruct((1, LANES), f32),
            jax.ShapeDtypeStruct((2, LANES), f32),
            jax.ShapeDtypeStruct((2, LANES), f32),
        ),
        in_specs=[VMEM] * (len(prepared) + len(received)),
        out_specs=(VMEM,) * 4,
        scratch_shapes=[pltpu.VMEM(kept, f32), pltpu.VMEM(kept, f32), pltpu.VMEM((4, LANES), f32)],
        cost_estimate=pl.CostEstimate(flops=COST[1], bytes_accessed=1 << 20, transcendentals=0),
        compiler_params=pltpu.CompilerParams(vmem_limit_bytes=6 * 2**20),
        name="patch_faces",
    )(*prepared, *received)


def group_faces_call(prepared, blocks, sums, rows, group, group_size, held):
    tiles = prepared[0].shape[1]
    bits = group.bit_length() - 1
    f32 = jnp.float32
    classes = tuple(range(blocks - 2))
    kept = (3, len(classes) * tiles // blocks, LANES)
    group_rows = [1] + [1 << bit for bit in range(bits)]
    return pl.pallas_call(
        lambda *refs: group_faces_kernel(classes, blocks, group, *refs),
        out_shape=(
            jax.ShapeDtypeStruct((rows, LANES), f32),
            *[jax.ShapeDtypeStruct((n, group_size), f32) for n in group_rows],
        ),
        in_specs=[VMEM] * (len(prepared) + 1 + len(held)),
        out_specs=(VMEM,) * (bits + 2),
        scratch_shapes=[
            pltpu.VMEM(kept, f32),
            pltpu.VMEM(kept, f32),
            pltpu.VMEM((8 * tiles + 32, LANES), f32),
            pltpu.VMEM((2 * len(classes), LANES), f32),
            pltpu.VMEM((2 * len(classes), LANES), f32),
        ],
        cost_estimate=pl.CostEstimate(flops=COST[1], bytes_accessed=1 << 20, transcendentals=0),
        compiler_params=pltpu.CompilerParams(vmem_limit_bytes=6 * 2**20),
        name="group_faces",
    )(*prepared, sums, *held)


def scatter_kernel(rows, bits, own_ref, sub_ref, pat_ref, direct_ref, outer_ref, inner_ref, *refs):
    out_ref = refs[-1]
    row_iota = iota((rows, LANES), 0)
    lane_iota = iota((LANES, LANES), 0)
    odd = jnp.broadcast_to(lax.axis_index("patch") & 1, (1, LANES)) == 1
    direct = direct_ref[0:1, :]
    below, above = by_side((lax.axis_index("patch") >> 1) & 1, outer_ref, inner_ref)
    group_back = refs[0][...]
    for i in range(bits):
        ref = refs[i + 1]
        for at in range(0, ref.shape[0], 1 << (bits - 1 - i)):
            group_back = group_back + ref[at : at + 1, :]
    backs = [
        group_back,
        jnp.where(odd, direct_ref[1:2, :], direct),
        above[0:1],
        jnp.where(odd, direct, direct_ref[1:2, :]),
        below[0:1],
    ]
    left, right = [], []
    for j in range(5):
        index = sub_ref[0:1, :] if j == 0 else pat_ref[j - 1 : j, :]
        value = backs[j]
        width = index.shape[1]
        hi = value.astype(jnp.bfloat16).astype(jnp.float32)
        match = jnp.broadcast_to(index >> 7, (rows, width)) == row_iota[:, :width]
        a_hi = jnp.where(match, jnp.broadcast_to(hi, (rows, width)), 0.0)
        a_lo = jnp.where(match, jnp.broadcast_to(value - hi, (rows, width)), 0.0)
        left.append(jnp.concatenate([a_hi, a_lo], axis=0).astype(jnp.bfloat16))
        spot = jnp.broadcast_to(index & (LANES - 1), (LANES, width)) == lane_iota[:, :width]
        right.append(jnp.where(spot, 1.0, 0.0).astype(jnp.bfloat16))
    product = 0.0
    for part in ([0], [1, 2, 3, 4]) if left[0].shape[1] < LANES else ([0, 1, 2, 3, 4],):
        product = product + lax.dot_general(
            jnp.concatenate([left[j] for j in part], axis=1),
            jnp.concatenate([right[j] for j in part], axis=1),
            (((1,), (1,)), ((), ())),
            preferred_element_type=jnp.float32,
        )
    out_ref[...] = own_ref[...] + product[:rows] + product[rows:]


def in_hbm(*arrays):
    return [pltpu.with_memory_space_constraint(array, pltpu.HBM) for array in arrays]


def stack(parts):
    return parts[0] if len(parts) == 1 else jnp.concatenate(parts, axis=0)


def per_device(heat, basis, area, corners, send_sub, send_pat, live_faces):
    owned = heat.shape[0]
    rows = owned // LANES
    group = lax.axis_size("sub")
    group_size = send_sub.shape[0]
    block_size = send_pat.shape[1]
    offsets = send_pat.shape[0]
    remote_len = group * group_size + offsets * block_size
    assert offsets == 4 and block_size == LANES and LANES % group_size == 0
    assert group & (group - 1) == 0 and group * group_size % (2 * LANES) == 0
    assert lax.axis_size("patch") % 4 == 0
    bits = group.bit_length() - 1
    f32 = jnp.float32
    heat2 = heat.reshape(rows, LANES)
    sub2 = send_sub.reshape(1, group_size)

    mine, near, outer, inner, sub_index, pat_index = pl.pallas_call(
        lambda *refs: send_kernel(rows, *refs),
        out_shape=(
            jax.ShapeDtypeStruct((1, group_size), f32),
            jax.ShapeDtypeStruct((1, LANES), f32),
            jax.ShapeDtypeStruct((2, LANES), f32),
            jax.ShapeDtypeStruct((2, LANES), f32),
            jax.ShapeDtypeStruct(sub2.shape, jnp.int32),
            jax.ShapeDtypeStruct(send_pat.shape, jnp.int32),
        ),
        in_specs=[HBM] * 3,
        out_specs=(VMEM,) * 6,
        scratch_shapes=[
            pltpu.VMEM(heat2.shape, f32),
            pltpu.SemaphoreType.DMA((3,)),
        ],
        compiler_params=pltpu.CompilerParams(vmem_limit_bytes=2 * 2**20),
        name="send_gather",
    )(*in_hbm(heat2, sub2, send_pat))
    blocks = remote_len // (2 * LANES)
    prepared = prepare_call(live_faces, heat2, corners, basis, area, blocks)
    place = lax.axis_index("patch")
    take_inner = ((place >> 1) & 1) == (place & 1)
    outer = swap_far(outer, "patch", True)
    inner = swap_far(inner, "patch", False)
    relay = jnp.where(take_inner, inner[1:2], outer[1:2])
    direct = swap(jnp.concatenate([near, relay]), "patch", 1)
    held = [mine]
    for bit in range(bits):
        held.append(swap(stack(held), "sub", 1 << bit))

    sums, near, outer, inner = patch_faces_call(prepared, blocks, (direct, outer, inner))
    own_sums, keep, *outs = group_faces_call(prepared, blocks, sums, rows, group, group_size, held)

    outer = swap_far(outer, "patch", True)
    inner = swap_far(inner, "patch", False)
    relay = jnp.where(take_inner, inner[1:2], outer[1:2])
    direct = swap(jnp.concatenate([near, relay]), "patch", 1)
    pieces, group_back = [], []
    for bit in reversed(range(bits)):
        width = 1 << bit
        got = swap(stack([outs[bit]] + [p[width : 2 * width] for p in pieces]), "sub", width)
        group_back.append(got)
        pieces = [p[:width] for p in pieces] + [
            got[at : at + width] for at in range(0, got.shape[0], width)
        ]

    result = pl.pallas_call(
        lambda *refs: scatter_kernel(rows, bits, *refs),
        out_shape=jax.ShapeDtypeStruct((rows, LANES), f32),
        in_specs=[VMEM] * (7 + bits),
        out_specs=VMEM,
        compiler_params=pltpu.CompilerParams(vmem_limit_bytes=4 * 2**20),
        name="scatter_back",
    )(own_sums, sub_index, pat_index, direct, outer, inner, keep, *group_back)
    return result.reshape(-1)


def solution(mesh):
    placed = (
        P(("patch", "sub")),
        P(None, ("patch", "sub")),
        P(("patch", "sub")),
        P(None, ("patch", "sub")),
        P(("patch", "sub")),
        P(None, ("patch", "sub")),
        P(("patch", "sub")),
    )

    return jax.shard_map(per_device, mesh=mesh, in_specs=placed, out_specs=P(("patch", "sub")), check_vma=False)
```

```python
import jax
import jax.numpy as jnp
from jax import lax
from jax.experimental import pallas as pl
from jax.experimental.pallas import tpu as pltpu
from jax.sharding import PartitionSpec as P


LANES = 128
HALF = 64
QUARTER = 32
COST = (1 << 24, 1 << 24)
VMEM = pl.BlockSpec(memory_space=pltpu.VMEM)
HBM = pl.BlockSpec(memory_space=pltpu.HBM)
SMEM = pl.BlockSpec(memory_space=pltpu.SMEM)


def swap_far(x, axis, outer):
    n = lax.axis_size(axis)
    low = [i for i in range(n) if (i % 4 >= 2) == outer]
    return lax.ppermute(x, axis, [(i, (i + 2) % n) for i in low] + [((i + 2) % n, i) for i in low])


def swap(x, axis, bit):
    n = lax.axis_size(axis)
    return lax.ppermute(x, axis, [(i, i ^ bit) for i in range(n)])


def iota(shape, dim, dtype=jnp.int32):
    return lax.broadcasted_iota(jnp.int32, shape, dim).astype(dtype)


def lane_gather(table, lanes):
    return jnp.take_along_axis(table, lanes, axis=1, mode="promise_in_bounds")


def read(ref, at):
    return ref[pl.ds(at, 1), :]


def send_kernel(
    rows, heat_hbm, sub_hbm, pat_hbm, group_ref, near_ref, outer_ref, inner_ref, sub_ref, pat_ref, heat_ref, sems
):
    copies = [
        pltpu.make_async_copy(source, target, sems.at[i])
        for i, (source, target) in enumerate(((heat_hbm, heat_ref), (sub_hbm, sub_ref), (pat_hbm, pat_ref)))
    ]
    for copy in copies:
        copy.start()
    for copy in copies:
        copy.wait()
    blocks = rows // 8
    sub_iota = iota((8, LANES), 0)
    odd = lax.axis_index("patch") & 1
    high = (lax.axis_index("patch") >> 1) & 1
    for j in range(5):
        if j == 0:
            index = sub_ref[0:1, :]
        else:
            index = read(pat_ref, (3 - 2 * high, 1 + 2 * high, 2 * odd, 2 - 2 * odd)[j - 1])
        index = jnp.broadcast_to(index, (8, index.shape[1]))
        if index.shape[1] < LANES:
            index = jnp.concatenate([index] * (LANES // index.shape[1]), axis=1)
        lane = index & (LANES - 1)
        row = index >> 7
        total = jnp.zeros((8, LANES), jnp.float32)
        for a in range(blocks):
            got = lane_gather(heat_ref[8 * a : 8 * a + 8, :], lane)
            total = jnp.where(row == sub_iota + 8 * a, got, total)
        total = jnp.where((row & 7) == sub_iota, total, 0.0)
        total = jnp.sum(total, axis=0, keepdims=True)
        if j == 0:
            group_ref[...] = total[:, : sub_ref.shape[1]]
        elif j < 3:
            (outer_ref, inner_ref)[j - 1][0:1, :] = total
        elif j == 3:
            near_ref[...] = total
        else:
            outer_ref[1:2, :] = total
            inner_ref[1:2, :] = total


def by_side(high, outer_ref, inner_ref):
    is_high = jnp.broadcast_to(high, outer_ref.shape) == 1
    outer, inner = outer_ref[...], inner_ref[...]
    return jnp.where(is_high, inner, outer), jnp.where(is_high, outer, inner)


def prepare_kernel(
    owned,
    tiles,
    blocks,
    live_ref,
    heat_hbm,
    corner_hbm,
    basis_hbm,
    area_hbm,
    near_out,
    off_out,
    part_out,
    lane_out,
    basis_out,
    last_out,
    weight_out,
    heat_ref,
    corner_ref,
    basis_ref,
    area_ref,
    win,
    corner_s,
    sems,
):
    copies = [
        pltpu.make_async_copy(source, target, sems.at[i])
        for i, (source, target) in enumerate(
            ((corner_hbm, corner_ref), (heat_hbm, heat_ref), (basis_hbm, basis_ref), (area_hbm, area_ref))
        )
    ]
    for copy in copies:
        copy.start()
    rows = owned // LANES
    lane_iota = iota((8, LANES), 1)
    sub_iota = iota((8, LANES), 0)
    copies[1].wait()
    zero = jnp.zeros((8, LANES), jnp.float32)
    win[0:8, :] = zero
    win[2 * rows : 2 * rows + 8, :] = zero
    for a in range(rows // 8):
        here = heat_ref[8 * a : 8 * a + 8, :]
        if a + 1 < rows // 8:
            after = heat_ref[8 * a + 1 : 8 * a + 9, :]
        else:
            after = jnp.concatenate([heat_ref[8 * a + 1 : 8 * a + 8, :], zero[0:1]], axis=0)
        both = jnp.where(lane_iota < HALF, after, here)
        win[pl.ds(16 * a + 2, 8, stride=2), :] = here
        win[pl.ds(16 * a + 3, 8, stride=2), :] = pltpu.roll(both, HALF, 1)
    first = pltpu.roll(jnp.broadcast_to(heat_ref[0:1, :], (8, LANES)), HALF, 1)
    win[1:2, :] = jnp.where(lane_iota < HALF, 0.0, first)[0:1]
    copies[0].wait()

    per_class = tiles // blocks
    place = [t % blocks * per_class + t // blocks for t in range(tiles)]
    for t in range(tiles):
        corner_s[4 * place[t] : 4 * place[t] + 3, :] = corner_ref[:, LANES * t : LANES * (t + 1)]
    for r in range(blocks):
        for g in range(per_class // 8):
            t0 = 8 * blocks * g + r
            tile = t0 + blocks * sub_iota
            near = [win[pl.ds(t0 + 2 * i, 8, stride=blocks), :] for i in range(2)]
            near_start = HALF * tile - LANES
            far_start = owned + 2 * LANES * r - 2 * LANES
            at = slice(per_class * r + 8 * g, per_class * r + 8 * g + 8)
            for k in range(3):
                pos = corner_s[pl.ds(4 * (per_class * r + 8 * g) + k, 8, stride=4), :]
                off = pos - jnp.where(pos >= owned, far_start, near_start)
                lane = off & (LANES - 1)
                near_out[k, at, :] = jnp.where(
                    off >= LANES, lane_gather(near[1], lane), lane_gather(near[0], lane)
                )
                off_out[k, at, :] = off
                part_out[k, at, :] = (off >> 5).astype(jnp.float32)
                lane_out[k, at, :] = (off & (QUARTER - 1)).astype(jnp.float32)
    copies[2].wait()

    for t in range(tiles):
        nine = basis_ref[:, LANES * t : LANES * (t + 1)].astype(jnp.float32)
        basis_out[8 * place[t] : 8 * place[t] + 8, :] = nine[0:8]
        last_out[place[t] : place[t] + 1, :] = nine[8:9]
    copies[3].wait()
    live = live_ref[0]
    for r in range(blocks):
        for g in range(per_class // 8):
            t0 = 8 * blocks * g + r
            slot = (t0 + blocks * sub_iota) * LANES + lane_iota
            at = slice(per_class * r + 8 * g, per_class * r + 8 * g + 8)
            weight_out[at, :] = jnp.where(slot < live, -area_ref[pl.ds(t0, 8, stride=blocks), :], 0.0)


def prepare_call(live_faces, heat2, corners, basis, area, blocks):
    rows = heat2.shape[0]
    tiles = corners.shape[1] // LANES
    f32 = jnp.float32
    per_corner = (3, tiles, LANES)
    return pl.pallas_call(
        lambda *refs: prepare_kernel(rows * LANES, tiles, blocks, *refs),
        out_shape=(
            jax.ShapeDtypeStruct(per_corner, f32),
            jax.ShapeDtypeStruct(per_corner, jnp.int32),
            jax.ShapeDtypeStruct(per_corner, f32),
            jax.ShapeDtypeStruct(per_corner, f32),
            jax.ShapeDtypeStruct((8 * tiles, LANES), f32),
            jax.ShapeDtypeStruct((tiles, LANES), f32),
            jax.ShapeDtypeStruct((tiles, LANES), f32),
        ),
        in_specs=[SMEM] + [HBM] * 4,
        out_specs=(VMEM,) * 7,
        scratch_shapes=[
            pltpu.VMEM(heat2.shape, f32),
            pltpu.VMEM(corners.shape, jnp.int32),
            pltpu.VMEM(basis.shape, basis.dtype),
            pltpu.VMEM((tiles, LANES), f32),
            pltpu.VMEM((2 * rows + 8, LANES), f32),
            pltpu.VMEM((4 * tiles, LANES), jnp.int32),
            pltpu.SemaphoreType.DMA((4,)),
        ],
        cost_estimate=pl.CostEstimate(flops=COST[0], bytes_accessed=1 << 20, transcendentals=0),
        compiler_params=pltpu.CompilerParams(vmem_limit_bytes=6 * 2**20),
        name="prepare",
    )(live_faces, *in_hbm(heat2, corners, basis, area.reshape(tiles, LANES)))


def spread_row(ref, k, row, height):
    return jnp.broadcast_to(ref[k, row : row + 1, :], (height, LANES)).astype(jnp.bfloat16)


def lane_match(lane_ref, k, row):
    match = spread_row(lane_ref, k, row, QUARTER) == iota((QUARTER, LANES), 0, jnp.float32).astype(jnp.bfloat16)
    return jnp.where(match, jnp.ones(match.shape, jnp.bfloat16), jnp.zeros(match.shape, jnp.bfloat16))


def contract(left, right):
    return lax.dot_general(
        jnp.concatenate(left, axis=1),
        jnp.concatenate(right, axis=1),
        (((1,), (1,)), ((), ())),
        preferred_element_type=jnp.float32,
    )


def window_part(first, part_ref, hi_ref, lo_ref, k, row, kept):
    want = (first + (iota((16, LANES), 0) & 7)).astype(jnp.float32).astype(jnp.bfloat16)
    value = jnp.concatenate(
        [jnp.broadcast_to(ref[k, kept : kept + 1, :], (8, LANES)) for ref in (hi_ref, lo_ref)], axis=0
    ).astype(jnp.bfloat16)
    return jnp.where(spread_row(part_ref, k, row, 16) == want, value, jnp.zeros((16, LANES), jnp.bfloat16))


def class_terms(classes, blocks, prepared, remote_ref, hi_s, lo_s):
    near_ref, off_ref, _, _, basis_s, last_s, weight_ref = prepared
    per_class = near_ref.shape[1] // blocks
    for r in classes:
        far_rows = [
            jnp.broadcast_to(remote_ref[2 * (r - classes[0]) + i : 2 * (r - classes[0]) + i + 1, :], (8, LANES))
            for i in range(2)
        ]
        for g in range(per_class // 8):
            row = per_class * r + 8 * g
            at = slice(row, row + 8)
            values = []
            for k in range(3):
                off = off_ref[k, at, :]
                lane = off & (LANES - 1)
                far = jnp.where(
                    off >= 3 * LANES, lane_gather(far_rows[1], lane), lane_gather(far_rows[0], lane)
                )
                values.append(jnp.where(off >= 2 * LANES, far, near_ref[k, at, :]))
            basis = [basis_s[pl.ds(8 * row + i, 8, stride=8), :] for i in range(8)] + [last_s[at, :]]
            grad = [sum(basis[3 * k + c] * values[k] for k in range(3)) for c in range(3)]
            square = grad[0] * grad[0] + grad[1] * grad[1] + grad[2] * grad[2]
            scale = weight_ref[at, :] / jnp.maximum(jnp.sqrt(square), 1.0)
            field = [grad[c] * scale for c in range(3)]
            kept = slice(row - per_class * classes[0], row - per_class * classes[0] + 8)
            for k in range(3):
                term = sum(basis[3 * k + c] * field[c] for c in range(3))
                hi = term.astype(jnp.bfloat16).astype(jnp.float32)
                hi_s[k, kept, :] = hi
                lo_s[k, kept, :] = term - hi


def remote_sums(classes, per_class, part_ref, lane_ref, hi_s, lo_s):
    found = []
    for r in classes:
        total = jnp.zeros((16, QUARTER), jnp.float32)
        for i in range(0, per_class, 2):
            rows = [(k, per_class * r + i + t) for t in range(2) for k in range(3)]
            left = [window_part(8, part_ref, hi_s, lo_s, k, row, row - per_class * classes[0]) for k, row in rows]
            total = total + contract(left, [lane_match(lane_ref, k, row) for k, row in rows])
        found.append(total[:8] + total[8:])
    return found


def owned_sums(classes, blocks, per_class, part_ref, lane_ref, hi_ref, lo_ref, sums_s):
    for r in classes:
        for i in range(per_class):
            row = per_class * r + i
            kept = row - per_class * classes[0]
            left = [window_part(0, part_ref, hi_ref, lo_ref, k, row, kept) for k in range(3)]
            total = contract(left, [lane_match(lane_ref, k, row) for k in range(3)])
            spot = 8 * (blocks * i + r) + 8
            sums_s[spot : spot + 8, 0:QUARTER] = total[:8] + total[8:]


def both_sums(classes, blocks, per_class, part_ref, lane_ref, hi_s, lo_s, sums_s):
    part_row = iota((16, LANES), 0, jnp.float32).astype(jnp.bfloat16)
    nil = jnp.zeros((16, LANES), jnp.bfloat16)
    found = []
    for r in classes:
        remote_sum = jnp.zeros((8, QUARTER), jnp.float32)
        for i in range(per_class):
            row = per_class * r + i
            kept = row - per_class * classes[0]
            left = []
            for k in range(3):
                match = spread_row(part_ref, k, row, 16) == part_row
                parts = [jnp.where(match, spread_row(ref, k, kept, 16), nil) for ref in (hi_s, lo_s)]
                left.append(jnp.concatenate(parts, axis=0))
            product = contract(left, [lane_match(lane_ref, k, row) for k in range(3)])
            total = product[:16] + product[16:]
            spot = 8 * (blocks * i + r) + 8
            sums_s[spot : spot + 8, 0:QUARTER] = total[:8]
            remote_sum = remote_sum + total[8:]
        found.append(remote_sum)
    return found


def full_rows(quarters):
    return [
        jnp.concatenate([sums[4 * i + e : 4 * i + e + 1] for e in range(4)], axis=1)
        for sums in quarters
        for i in range(2)
    ]


def patch_faces_kernel(classes, blocks, *refs):
    prepared, refs = refs[:7], refs[7:]
    direct_ref, outer_ref, inner_ref, hi_out, lo_out, near_out, outer_out, inner_out, remote_ref = refs
    per_class = prepared[0].shape[1] // blocks
    odd = lax.axis_index("patch") & 1
    high = (lax.axis_index("patch") >> 1) & 1
    is_odd = jnp.broadcast_to(odd, (1, LANES)) == 1
    is_high = jnp.broadcast_to(high, (1, LANES)) == 1
    direct = direct_ref[0:1, :]
    below, above = by_side(high, outer_ref, inner_ref)
    relayed = direct_ref[1:2, :]
    remote_ref[0:1, :] = jnp.where(is_odd, direct, relayed)
    remote_ref[1:2, :] = below[0:1]
    remote_ref[2:3, :] = jnp.where(is_odd, relayed, direct)
    remote_ref[3:4, :] = above[0:1]
    class_terms(classes, blocks, prepared, remote_ref, hi_out, lo_out)
    rows = full_rows(remote_sums(classes, per_class, prepared[2], prepared[3], hi_out, lo_out))
    outer_out[0:1, :] = jnp.where(is_high, rows[3], rows[1])
    inner_out[0:1, :] = jnp.where(is_high, rows[1], rows[3])
    near_out[...] = jnp.where(is_odd, rows[0], rows[2])
    relay = jnp.where(is_odd, rows[2], rows[0])
    outer_out[1:2, :] = relay
    inner_out[1:2, :] = relay


def group_faces_kernel(classes, blocks, group, *refs):
    prepared, patch_hi, patch_lo, refs = refs[:7], refs[7], refs[8], refs[9:]
    per_class = prepared[0].shape[1] // blocks
    tiles = prepared[0].shape[1]
    bits = group.bit_length() - 1
    group_refs = refs[: bits + 1]
    own_out, group_keep, *group_outs = refs[bits + 1 : 2 * bits + 3]
    hi_s, lo_s, sums_s, remote_ref, remote_out = refs[2 * bits + 3 :]
    group_size = group_keep.shape[1]
    me = lax.axis_index("sub")
    rows = own_out.shape[0]
    lane_iota = iota((8, LANES), 1)
    per_row = LANES // group_size
    for q in range(group // per_row):
        parts = []
        for e in range(per_row):
            from_me = me ^ (q * per_row + e)
            part = group_refs[0][...]
            for bit in range(bits):
                got = read(group_refs[bit + 1], from_me & ((1 << bit) - 1))
                part = jnp.where(from_me >> bit == 1, got, part)
            parts.append(part)
        remote_ref[q : q + 1, :] = parts[0] if per_row == 1 else jnp.concatenate(parts, axis=1)
    sums_s[0:8, :] = jnp.zeros((8, LANES), jnp.float32)
    sums_s[8 * tiles + 8 : 8 * tiles + 32, :] = jnp.zeros((24, LANES), jnp.float32)
    class_terms(classes, blocks, prepared, remote_ref, hi_s, lo_s)
    part_ref, lane_ref = prepared[2:4]
    found = both_sums(classes, blocks, per_class, part_ref, lane_ref, hi_s, lo_s, sums_s)
    for i, row in enumerate(full_rows(found)):
        remote_out[i : i + 1, :] = row
    others = tuple(r for r in range(blocks) if r not in classes)
    owned_sums(others, blocks, per_class, part_ref, lane_ref, patch_hi, patch_lo, sums_s)
    for i in range(group):
        owner = me ^ i
        row = read(remote_out, owner // per_row)
        if per_row > 1:
            turn = (LANES - (owner % per_row) * group_size) % LANES
            row = pltpu.roll(jnp.broadcast_to(row, (8, LANES)), turn, 1)[0:1, :group_size]
        if i == 0:
            group_keep[...] = row
        else:
            bit = i.bit_length() - 1
            group_outs[bit][i - (1 << bit) : i - (1 << bit) + 1, :] = row
    for a in range(rows // 8):
        whole = None
        for e in range(4):
            total = None
            for h in range(e & 1, 8, 2):
                tile = 16 * a + (e + 4 - h) // 2
                got = sums_s[pl.ds(8 * (tile + 1) + h, 8, stride=16), :]
                total = got if total is None else total + got
            if e == 0:
                whole = total
            else:
                whole = jnp.where(lane_iota >= QUARTER * e, pltpu.roll(total, QUARTER * e, 1), whole)
        own_out[8 * a : 8 * a + 8, :] = whole


def patch_faces_call(prepared, blocks, received):
    tiles = prepared[0].shape[1]
    f32 = jnp.float32
    classes = tuple(range(blocks - 2, blocks))
    kept = (3, 2 * tiles // blocks, LANES)
    return pl.pallas_call(
        lambda *refs: patch_faces_kernel(classes, blocks, *refs),
        out_shape=(
            jax.ShapeDtypeStruct(kept, f32),
            jax.ShapeDtypeStruct(kept, f32),
            jax.ShapeDtypeStruct((1, LANES), f32),
            jax.ShapeDtypeStruct((2, LANES), f32),
            jax.ShapeDtypeStruct((2, LANES), f32),
        ),
        in_specs=[VMEM] * (len(prepared) + len(received)),
        out_specs=(VMEM,) * 5,
        scratch_shapes=[pltpu.VMEM((4, LANES), f32)],
        cost_estimate=pl.CostEstimate(flops=COST[1], bytes_accessed=1 << 20, transcendentals=0),
        compiler_params=pltpu.CompilerParams(vmem_limit_bytes=6 * 2**20),
        name="patch_faces",
    )(*prepared, *received)


def group_faces_call(prepared, blocks, patch_terms, rows, group, group_size, held):
    tiles = prepared[0].shape[1]
    bits = group.bit_length() - 1
    f32 = jnp.float32
    classes = tuple(range(blocks - 2))
    kept = (3, len(classes) * tiles // blocks, LANES)
    group_rows = [1] + [1 << bit for bit in range(bits)]
    return pl.pallas_call(
        lambda *refs: group_faces_kernel(classes, blocks, group, *refs),
        out_shape=(
            jax.ShapeDtypeStruct((rows, LANES), f32),
            *[jax.ShapeDtypeStruct((n, group_size), f32) for n in group_rows],
        ),
        in_specs=[VMEM] * (len(prepared) + 2 + len(held)),
        out_specs=(VMEM,) * (bits + 2),
        scratch_shapes=[
            pltpu.VMEM(kept, f32),
            pltpu.VMEM(kept, f32),
            pltpu.VMEM((8 * tiles + 32, LANES), f32),
            pltpu.VMEM((2 * len(classes), LANES), f32),
            pltpu.VMEM((2 * len(classes), LANES), f32),
        ],
        cost_estimate=pl.CostEstimate(flops=COST[1], bytes_accessed=1 << 20, transcendentals=0),
        compiler_params=pltpu.CompilerParams(vmem_limit_bytes=6 * 2**20),
        name="group_faces",
    )(*prepared, *patch_terms, *held)


def scatter_kernel(rows, bits, own_ref, sub_ref, pat_ref, direct_ref, outer_ref, inner_ref, *refs):
    out_ref = refs[-1]
    row_iota = iota((rows, LANES), 0)
    lane_iota = iota((LANES, LANES), 0)
    odd = jnp.broadcast_to(lax.axis_index("patch") & 1, (1, LANES)) == 1
    direct = direct_ref[0:1, :]
    below, above = by_side((lax.axis_index("patch") >> 1) & 1, outer_ref, inner_ref)
    group_back = refs[0][...]
    for i in range(bits):
        ref = refs[i + 1]
        for at in range(0, ref.shape[0], 1 << (bits - 1 - i)):
            group_back = group_back + ref[at : at + 1, :]
    backs = [
        group_back,
        jnp.where(odd, direct_ref[1:2, :], direct),
        above[0:1],
        jnp.where(odd, direct, direct_ref[1:2, :]),
        below[0:1],
    ]
    left, right = [], []
    for j in range(5):
        index = sub_ref[0:1, :] if j == 0 else pat_ref[j - 1 : j, :]
        value = backs[j]
        width = index.shape[1]
        hi = value.astype(jnp.bfloat16).astype(jnp.float32)
        match = jnp.broadcast_to(index >> 7, (rows, width)) == row_iota[:, :width]
        a_hi = jnp.where(match, jnp.broadcast_to(hi, (rows, width)), 0.0)
        a_lo = jnp.where(match, jnp.broadcast_to(value - hi, (rows, width)), 0.0)
        left.append(jnp.concatenate([a_hi, a_lo], axis=0).astype(jnp.bfloat16))
        spot = jnp.broadcast_to(index & (LANES - 1), (LANES, width)) == lane_iota[:, :width]
        right.append(jnp.where(spot, 1.0, 0.0).astype(jnp.bfloat16))
    product = 0.0
    for part in ([0], [1, 2, 3, 4]) if left[0].shape[1] < LANES else ([0, 1, 2, 3, 4],):
        product = product + lax.dot_general(
            jnp.concatenate([left[j] for j in part], axis=1),
            jnp.concatenate([right[j] for j in part], axis=1),
            (((1,), (1,)), ((), ())),
            preferred_element_type=jnp.float32,
        )
    out_ref[...] = own_ref[...] + product[:rows] + product[rows:]


def in_hbm(*arrays):
    return [pltpu.with_memory_space_constraint(array, pltpu.HBM) for array in arrays]


def stack(parts):
    return parts[0] if len(parts) == 1 else jnp.concatenate(parts, axis=0)


def per_device(heat, basis, area, corners, send_sub, send_pat, live_faces):
    owned = heat.shape[0]
    rows = owned // LANES
    group = lax.axis_size("sub")
    group_size = send_sub.shape[0]
    block_size = send_pat.shape[1]
    offsets = send_pat.shape[0]
    remote_len = group * group_size + offsets * block_size
    assert offsets == 4 and block_size == LANES and LANES % group_size == 0
    assert group & (group - 1) == 0 and group * group_size % (2 * LANES) == 0
    assert lax.axis_size("patch") % 4 == 0
    bits = group.bit_length() - 1
    f32 = jnp.float32
    heat2 = heat.reshape(rows, LANES)
    sub2 = send_sub.reshape(1, group_size)

    mine, near, outer, inner, sub_index, pat_index = pl.pallas_call(
        lambda *refs: send_kernel(rows, *refs),
        out_shape=(
            jax.ShapeDtypeStruct((1, group_size), f32),
            jax.ShapeDtypeStruct((1, LANES), f32),
            jax.ShapeDtypeStruct((2, LANES), f32),
            jax.ShapeDtypeStruct((2, LANES), f32),
            jax.ShapeDtypeStruct(sub2.shape, jnp.int32),
            jax.ShapeDtypeStruct(send_pat.shape, jnp.int32),
        ),
        in_specs=[HBM] * 3,
        out_specs=(VMEM,) * 6,
        scratch_shapes=[
            pltpu.VMEM(heat2.shape, f32),
            pltpu.SemaphoreType.DMA((3,)),
        ],
        compiler_params=pltpu.CompilerParams(vmem_limit_bytes=2 * 2**20),
        name="send_gather",
    )(*in_hbm(heat2, sub2, send_pat))
    blocks = remote_len // (2 * LANES)
    prepared = prepare_call(live_faces, heat2, corners, basis, area, blocks)
    place = lax.axis_index("patch")
    take_inner = ((place >> 1) & 1) == (place & 1)
    outer = swap_far(outer, "patch", True)
    inner = swap_far(inner, "patch", False)
    relay = jnp.where(take_inner, inner[1:2], outer[1:2])
    direct = swap(jnp.concatenate([near, relay]), "patch", 1)
    held = [mine]
    for bit in range(bits):
        held.append(swap(stack(held), "sub", 1 << bit))

    *patch_terms, near, outer, inner = patch_faces_call(prepared, blocks, (direct, outer, inner))
    own_sums, keep, *outs = group_faces_call(prepared, blocks, patch_terms, rows, group, group_size, held)

    outer = swap_far(outer, "patch", True)
    inner = swap_far(inner, "patch", False)
    relay = jnp.where(take_inner, inner[1:2], outer[1:2])
    direct = swap(jnp.concatenate([near, relay]), "patch", 1)
    pieces, group_back = [], []
    for bit in reversed(range(bits)):
        width = 1 << bit
        got = swap(stack([outs[bit]] + [p[width : 2 * width] for p in pieces]), "sub", width)
        group_back.append(got)
        pieces = [p[:width] for p in pieces] + [
            got[at : at + width] for at in range(0, got.shape[0], width)
        ]

    result = pl.pallas_call(
        lambda *refs: scatter_kernel(rows, bits, *refs),
        out_shape=jax.ShapeDtypeStruct((rows, LANES), f32),
        in_specs=[VMEM] * (7 + bits),
        out_specs=VMEM,
        compiler_params=pltpu.CompilerParams(vmem_limit_bytes=4 * 2**20),
        name="scatter_back",
    )(own_sums, sub_index, pat_index, direct, outer, inner, keep, *group_back)
    return result.reshape(-1)


def solution(mesh):
    placed = (
        P(("patch", "sub")),
        P(None, ("patch", "sub")),
        P(("patch", "sub")),
        P(None, ("patch", "sub")),
        P(("patch", "sub")),
        P(None, ("patch", "sub")),
        P(("patch", "sub")),
    )

    return jax.shard_map(per_device, mesh=mesh, in_specs=placed, out_specs=P(("patch", "sub")), check_vma=False)
```

```python
import jax
import jax.numpy as jnp
from jax import lax
from jax.experimental import pallas as pl
from jax.experimental.pallas import tpu as pltpu
from jax.sharding import PartitionSpec as P


LANES = 128
HALF = 64
QUARTER = 32
COST = (1 << 24, 1 << 24)
VMEM = pl.BlockSpec(memory_space=pltpu.VMEM)
HBM = pl.BlockSpec(memory_space=pltpu.HBM)
SMEM = pl.BlockSpec(memory_space=pltpu.SMEM)


def swap_far(x, axis, outer):
    n = lax.axis_size(axis)
    low = [i for i in range(n) if (i % 4 >= 2) == outer]
    return lax.ppermute(x, axis, [(i, (i + 2) % n) for i in low] + [((i + 2) % n, i) for i in low])


def swap(x, axis, mask):
    n = lax.axis_size(axis)
    return lax.ppermute(x, axis, [(i, i ^ mask) for i in range(n)])


def mask_of(bit):
    return (2 << bit) - 1


def owner_of(i):
    mask, bit = 0, 0
    while i >> bit:
        mask ^= mask_of(bit) if i >> bit & 1 else 0
        bit += 1
    return mask


def shift(x, axis, by):
    n = lax.axis_size(axis)
    return lax.ppermute(x, axis, [(i, (i + by) % n) for i in range(n)])


def iota(shape, dim, dtype=jnp.int32):
    return lax.broadcasted_iota(jnp.int32, shape, dim).astype(dtype)


def lane_gather(table, lanes):
    return jnp.take_along_axis(table, lanes, axis=1, mode="promise_in_bounds")


def read(ref, at):
    return ref[pl.ds(at, 1), :]


def send_kernel(
    rows, heat_hbm, sub_hbm, pat_hbm, group_ref, near_ref, outer_ref, inner_ref, sub_ref, pat_ref, heat_ref, sems
):
    copies = [
        pltpu.make_async_copy(source, target, sems.at[i])
        for i, (source, target) in enumerate(((heat_hbm, heat_ref), (sub_hbm, sub_ref), (pat_hbm, pat_ref)))
    ]
    for copy in copies:
        copy.start()
    copies[1].wait()
    copies[2].wait()
    blocks = rows // 8
    sub_iota = iota((8, LANES), 0)
    odd = lax.axis_index("patch") & 1
    wanted = []
    for j in range(5):
        if j == 0:
            index = sub_ref[0:1, :]
        else:
            index = read(pat_ref, (1, 3, 2 * odd, 2 - 2 * odd)[j - 1])
        index = jnp.broadcast_to(index, (8, index.shape[1]))
        if index.shape[1] < LANES:
            index = jnp.concatenate([index] * (LANES // index.shape[1]), axis=1)
        lane = index & (LANES - 1)
        row = index >> 7
        wanted.append((lane, row))
    copies[0].wait()
    for j, (lane, row) in enumerate(wanted):
        total = jnp.zeros((8, LANES), jnp.float32)
        for a in range(blocks):
            got = lane_gather(heat_ref[8 * a : 8 * a + 8, :], lane)
            total = jnp.where(row == sub_iota + 8 * a, got, total)
        total = jnp.where((row & 7) == sub_iota, total, 0.0)
        total = jnp.sum(total, axis=0, keepdims=True)
        if j == 0:
            group_ref[...] = total[:, : sub_ref.shape[1]]
        elif j < 3:
            (outer_ref, inner_ref)[j - 1][0:1, :] = total
        elif j == 3:
            near_ref[...] = total
        else:
            outer_ref[1:2, :] = total
            inner_ref[1:2, :] = total


def by_side(high, outer_ref, inner_ref):
    is_high = jnp.broadcast_to(high, outer_ref.shape) == 1
    outer, inner = outer_ref[...], inner_ref[...]
    return jnp.where(is_high, inner, outer), jnp.where(is_high, outer, inner)


def prepare_kernel(
    owned,
    tiles,
    blocks,
    live_ref,
    heat_hbm,
    corner_hbm,
    basis_hbm,
    area_hbm,
    near_out,
    off_out,
    part_out,
    lane_out,
    basis_out,
    last_out,
    weight_out,
    heat_ref,
    corner_ref,
    basis_ref,
    area_ref,
    win,
    corner_s,
    sems,
):
    copies = [
        pltpu.make_async_copy(source, target, sems.at[i])
        for i, (source, target) in enumerate(
            ((corner_hbm, corner_ref), (heat_hbm, heat_ref), (basis_hbm, basis_ref), (area_hbm, area_ref))
        )
    ]
    for copy in copies:
        copy.start()
    rows = owned // LANES
    lane_iota = iota((8, LANES), 1)
    sub_iota = iota((8, LANES), 0)
    copies[1].wait()
    zero = jnp.zeros((8, LANES), jnp.float32)
    win[0:8, :] = zero
    win[2 * rows : 2 * rows + 8, :] = zero
    for a in range(rows // 8):
        here = heat_ref[8 * a : 8 * a + 8, :]
        if a + 1 < rows // 8:
            after = heat_ref[8 * a + 1 : 8 * a + 9, :]
        else:
            after = jnp.concatenate([heat_ref[8 * a + 1 : 8 * a + 8, :], zero[0:1]], axis=0)
        both = jnp.where(lane_iota < HALF, after, here)
        win[pl.ds(16 * a + 2, 8, stride=2), :] = here
        win[pl.ds(16 * a + 3, 8, stride=2), :] = pltpu.roll(both, HALF, 1)
    first = pltpu.roll(jnp.broadcast_to(heat_ref[0:1, :], (8, LANES)), HALF, 1)
    win[1:2, :] = jnp.where(lane_iota < HALF, 0.0, first)[0:1]
    copies[0].wait()

    per_class = tiles // blocks
    place = [t % blocks * per_class + t // blocks for t in range(tiles)]
    for t in range(tiles):
        corner_s[4 * place[t] : 4 * place[t] + 3, :] = corner_ref[:, LANES * t : LANES * (t + 1)]
    for r in range(blocks):
        for g in range(per_class // 8):
            t0 = 8 * blocks * g + r
            tile = t0 + blocks * sub_iota
            near = [win[pl.ds(t0 + 2 * i, 8, stride=blocks), :] for i in range(2)]
            near_start = HALF * tile - LANES
            far_start = owned + 2 * LANES * r - 2 * LANES
            at = slice(per_class * r + 8 * g, per_class * r + 8 * g + 8)
            for k in range(3):
                pos = corner_s[pl.ds(4 * (per_class * r + 8 * g) + k, 8, stride=4), :]
                off = pos - jnp.where(pos >= owned, far_start, near_start)
                lane = off & (LANES - 1)
                near_out[k, at, :] = jnp.where(
                    off >= LANES, lane_gather(near[1], lane), lane_gather(near[0], lane)
                )
                off_out[k, at, :] = off
                part_out[k, at, :] = (off >> 5).astype(jnp.float32)
                lane_out[k, at, :] = (off & (QUARTER - 1)).astype(jnp.float32)
    copies[2].wait()

    for t in range(tiles):
        nine = basis_ref[:, LANES * t : LANES * (t + 1)].astype(jnp.float32)
        basis_out[8 * place[t] : 8 * place[t] + 8, :] = nine[0:8]
        last_out[place[t] : place[t] + 1, :] = nine[8:9]
    copies[3].wait()
    live = live_ref[0]
    for r in range(blocks):
        for g in range(per_class // 8):
            t0 = 8 * blocks * g + r
            slot = (t0 + blocks * sub_iota) * LANES + lane_iota
            at = slice(per_class * r + 8 * g, per_class * r + 8 * g + 8)
            weight_out[at, :] = jnp.where(slot < live, -area_ref[pl.ds(t0, 8, stride=blocks), :], 0.0)


def prepare_call(live_faces, heat2, corners, basis, area, blocks):
    rows = heat2.shape[0]
    tiles = corners.shape[1] // LANES
    f32 = jnp.float32
    per_corner = (3, tiles, LANES)
    return pl.pallas_call(
        lambda *refs: prepare_kernel(rows * LANES, tiles, blocks, *refs),
        out_shape=(
            jax.ShapeDtypeStruct(per_corner, f32),
            jax.ShapeDtypeStruct(per_corner, jnp.int32),
            jax.ShapeDtypeStruct(per_corner, f32),
            jax.ShapeDtypeStruct(per_corner, f32),
            jax.ShapeDtypeStruct((8 * tiles, LANES), f32),
            jax.ShapeDtypeStruct((tiles, LANES), f32),
            jax.ShapeDtypeStruct((tiles, LANES), f32),
        ),
        in_specs=[SMEM] + [HBM] * 4,
        out_specs=(VMEM,) * 7,
        scratch_shapes=[
            pltpu.VMEM(heat2.shape, f32),
            pltpu.VMEM(corners.shape, jnp.int32),
            pltpu.VMEM(basis.shape, basis.dtype),
            pltpu.VMEM((tiles, LANES), f32),
            pltpu.VMEM((2 * rows + 8, LANES), f32),
            pltpu.VMEM((4 * tiles, LANES), jnp.int32),
            pltpu.SemaphoreType.DMA((4,)),
        ],
        cost_estimate=pl.CostEstimate(flops=COST[0], bytes_accessed=1 << 20, transcendentals=0),
        compiler_params=pltpu.CompilerParams(vmem_limit_bytes=6 * 2**20),
        name="prepare",
    )(live_faces, *in_hbm(heat2, corners, basis, area.reshape(tiles, LANES)))


def spread_row(ref, k, row, height):
    return jnp.broadcast_to(ref[k, row : row + 1, :], (height, LANES)).astype(jnp.bfloat16)


def lane_match(lane_ref, k, row):
    match = spread_row(lane_ref, k, row, QUARTER) == iota((QUARTER, LANES), 0, jnp.float32).astype(jnp.bfloat16)
    return jnp.where(match, jnp.ones(match.shape, jnp.bfloat16), jnp.zeros(match.shape, jnp.bfloat16))


def contract(left, right):
    return lax.dot_general(
        jnp.concatenate(left, axis=1),
        jnp.concatenate(right, axis=1),
        (((1,), (1,)), ((), ())),
        preferred_element_type=jnp.float32,
    )


def window_part(first, part_ref, hi_ref, lo_ref, k, row, kept):
    want = (first + (iota((16, LANES), 0) & 7)).astype(jnp.float32).astype(jnp.bfloat16)
    value = jnp.concatenate(
        [jnp.broadcast_to(ref[k, kept : kept + 1, :], (8, LANES)) for ref in (hi_ref, lo_ref)], axis=0
    ).astype(jnp.bfloat16)
    return jnp.where(spread_row(part_ref, k, row, 16) == want, value, jnp.zeros((16, LANES), jnp.bfloat16))


def class_terms(classes, blocks, prepared, remote_ref, hi_s, lo_s):
    near_ref, off_ref, _, _, basis_s, last_s, weight_ref = prepared
    per_class = near_ref.shape[1] // blocks
    for r in classes:
        far_rows = [
            jnp.broadcast_to(remote_ref[2 * (r - classes[0]) + i : 2 * (r - classes[0]) + i + 1, :], (8, LANES))
            for i in range(2)
        ]
        for g in range(per_class // 8):
            row = per_class * r + 8 * g
            at = slice(row, row + 8)
            values = []
            for k in range(3):
                off = off_ref[k, at, :]
                lane = off & (LANES - 1)
                far = jnp.where(
                    off >= 3 * LANES, lane_gather(far_rows[1], lane), lane_gather(far_rows[0], lane)
                )
                values.append(jnp.where(off >= 2 * LANES, far, near_ref[k, at, :]))
            basis = [basis_s[pl.ds(8 * row + i, 8, stride=8), :] for i in range(8)] + [last_s[at, :]]
            grad = [sum(basis[3 * k + c] * values[k] for k in range(3)) for c in range(3)]
            square = grad[0] * grad[0] + grad[1] * grad[1] + grad[2] * grad[2]
            scale = weight_ref[at, :] / jnp.maximum(jnp.sqrt(square), 1.0)
            field = [grad[c] * scale for c in range(3)]
            kept = slice(row - per_class * classes[0], row - per_class * classes[0] + 8)
            for k in range(3):
                term = sum(basis[3 * k + c] * field[c] for c in range(3))
                hi = term.astype(jnp.bfloat16).astype(jnp.float32)
                hi_s[k, kept, :] = hi
                lo_s[k, kept, :] = term - hi


def remote_sums(classes, per_class, part_ref, lane_ref, hi_s, lo_s):
    found = []
    for r in classes:
        total = jnp.zeros((16, QUARTER), jnp.float32)
        for i in range(0, per_class, 2):
            rows = [(k, per_class * r + i + t) for t in range(2) for k in range(3)]
            left = [window_part(8, part_ref, hi_s, lo_s, k, row, row - per_class * classes[0]) for k, row in rows]
            total = total + contract(left, [lane_match(lane_ref, k, row) for k, row in rows])
        found.append(total[:8] + total[8:])
    return found


def owned_sums(classes, blocks, per_class, part_ref, lane_ref, hi_ref, lo_ref, sums_s):
    for r in classes:
        for i in range(per_class):
            row = per_class * r + i
            kept = row - per_class * classes[0]
            left = [window_part(0, part_ref, hi_ref, lo_ref, k, row, kept) for k in range(3)]
            total = contract(left, [lane_match(lane_ref, k, row) for k in range(3)])
            spot = 8 * (blocks * i + r) + 8
            sums_s[spot : spot + 8, 0:QUARTER] = total[:8] + total[8:]


def both_sums(classes, blocks, per_class, part_ref, lane_ref, hi_s, lo_s, sums_s):
    part_row = iota((16, LANES), 0, jnp.float32).astype(jnp.bfloat16)
    nil = jnp.zeros((16, LANES), jnp.bfloat16)
    found = []
    for r in classes:
        remote_sum = jnp.zeros((8, QUARTER), jnp.float32)
        for i in range(per_class):
            row = per_class * r + i
            kept = row - per_class * classes[0]
            left = []
            for k in range(3):
                match = spread_row(part_ref, k, row, 16) == part_row
                parts = [jnp.where(match, spread_row(ref, k, kept, 16), nil) for ref in (hi_s, lo_s)]
                left.append(jnp.concatenate(parts, axis=0))
            product = contract(left, [lane_match(lane_ref, k, row) for k in range(3)])
            total = product[:16] + product[16:]
            spot = 8 * (blocks * i + r) + 8
            sums_s[spot : spot + 8, 0:QUARTER] = total[:8]
            remote_sum = remote_sum + total[8:]
        found.append(remote_sum)
    return found


def full_rows(quarters):
    return [
        jnp.concatenate([sums[4 * i + e : 4 * i + e + 1] for e in range(4)], axis=1)
        for sums in quarters
        for i in range(2)
    ]


def patch_faces_kernel(classes, blocks, *refs):
    prepared, refs = refs[:7], refs[7:]
    direct_ref, outer_ref, inner_ref, hi_out, lo_out, near_out, outer_out, inner_out, remote_ref = refs
    per_class = prepared[0].shape[1] // blocks
    odd = lax.axis_index("patch") & 1
    high = (lax.axis_index("patch") >> 1) & 1
    is_odd = jnp.broadcast_to(odd, (1, LANES)) == 1
    is_high = jnp.broadcast_to(high, (1, LANES)) == 1
    direct = direct_ref[0:1, :]
    below, above = outer_ref[...], inner_ref[...]
    relayed = direct_ref[1:2, :]
    remote_ref[0:1, :] = jnp.where(is_odd, direct, relayed)
    remote_ref[1:2, :] = below[0:1]
    remote_ref[2:3, :] = jnp.where(is_odd, relayed, direct)
    remote_ref[3:4, :] = above[0:1]
    class_terms(classes, blocks, prepared, remote_ref, hi_out, lo_out)
    rows = full_rows(remote_sums(classes, per_class, prepared[2], prepared[3], hi_out, lo_out))
    outer_out[0:1, :] = jnp.where(is_high, rows[3], rows[1])
    inner_out[0:1, :] = jnp.where(is_high, rows[1], rows[3])
    near_out[...] = jnp.where(is_odd, rows[0], rows[2])
    relay = jnp.where(is_odd, rows[2], rows[0])
    outer_out[1:2, :] = relay
    inner_out[1:2, :] = relay


def group_faces_kernel(classes, blocks, group, *refs):
    prepared, patch_hi, patch_lo, refs = refs[:7], refs[7], refs[8], refs[9:]
    per_class = prepared[0].shape[1] // blocks
    tiles = prepared[0].shape[1]
    bits = group.bit_length() - 1
    group_refs = refs[: bits + 1]
    own_out, group_keep, *group_outs = refs[bits + 1 : 2 * bits + 3]
    hi_s, lo_s, sums_s, remote_ref, remote_out = refs[2 * bits + 3 :]
    group_size = group_keep.shape[1]
    me = lax.axis_index("sub")
    rows = own_out.shape[0]
    lane_iota = iota((8, LANES), 1)
    per_row = LANES // group_size
    for q in range(group // per_row):
        parts = []
        for e in range(per_row):
            from_me = me ^ (q * per_row + e)
            from_me = from_me ^ (from_me >> 1)
            part = group_refs[0][...]
            for bit in range(bits):
                got = read(group_refs[bit + 1], from_me & ((1 << bit) - 1))
                part = jnp.where(from_me >> bit == 1, got, part)
            parts.append(part)
        remote_ref[q : q + 1, :] = parts[0] if per_row == 1 else jnp.concatenate(parts, axis=1)
    sums_s[0:8, :] = jnp.zeros((8, LANES), jnp.float32)
    sums_s[8 * tiles + 8 : 8 * tiles + 32, :] = jnp.zeros((24, LANES), jnp.float32)
    class_terms(classes, blocks, prepared, remote_ref, hi_s, lo_s)
    part_ref, lane_ref = prepared[2:4]
    found = both_sums(classes, blocks, per_class, part_ref, lane_ref, hi_s, lo_s, sums_s)
    for i, row in enumerate(full_rows(found)):
        remote_out[i : i + 1, :] = row
    others = tuple(r for r in range(blocks) if r not in classes)
    owned_sums(others, blocks, per_class, part_ref, lane_ref, patch_hi, patch_lo, sums_s)
    for i in range(group):
        owner = me ^ owner_of(i)
        row = read(remote_out, owner // per_row)
        if per_row > 1:
            turn = (LANES - (owner % per_row) * group_size) % LANES
            row = pltpu.roll(jnp.broadcast_to(row, (8, LANES)), turn, 1)[0:1, :group_size]
        if i == 0:
            group_keep[...] = row
        else:
            bit = i.bit_length() - 1
            group_outs[bit][i - (1 << bit) : i - (1 << bit) + 1, :] = row
    for a in range(rows // 8):
        whole = None
        for e in range(4):
            total = None
            for h in range(e & 1, 8, 2):
                tile = 16 * a + (e + 4 - h) // 2
                got = sums_s[pl.ds(8 * (tile + 1) + h, 8, stride=16), :]
                total = got if total is None else total + got
            if e == 0:
                whole = total
            else:
                whole = jnp.where(lane_iota >= QUARTER * e, pltpu.roll(total, QUARTER * e, 1), whole)
        own_out[8 * a : 8 * a + 8, :] = whole


def patch_faces_call(prepared, blocks, received):
    tiles = prepared[0].shape[1]
    f32 = jnp.float32
    classes = tuple(range(blocks - 2, blocks))
    kept = (3, 2 * tiles // blocks, LANES)
    return pl.pallas_call(
        lambda *refs: patch_faces_kernel(classes, blocks, *refs),
        out_shape=(
            jax.ShapeDtypeStruct(kept, f32),
            jax.ShapeDtypeStruct(kept, f32),
            jax.ShapeDtypeStruct((1, LANES), f32),
            jax.ShapeDtypeStruct((2, LANES), f32),
            jax.ShapeDtypeStruct((2, LANES), f32),
        ),
        in_specs=[VMEM] * (len(prepared) + len(received)),
        out_specs=(VMEM,) * 5,
        scratch_shapes=[pltpu.VMEM((4, LANES), f32)],
        cost_estimate=pl.CostEstimate(flops=COST[1], bytes_accessed=1 << 20, transcendentals=0),
        compiler_params=pltpu.CompilerParams(vmem_limit_bytes=6 * 2**20),
        name="patch_faces",
    )(*prepared, *received)


def group_faces_call(prepared, blocks, patch_terms, rows, group, group_size, held):
    tiles = prepared[0].shape[1]
    bits = group.bit_length() - 1
    f32 = jnp.float32
    classes = tuple(range(blocks - 2))
    kept = (3, len(classes) * tiles // blocks, LANES)
    group_rows = [1] + [1 << bit for bit in range(bits)]
    return pl.pallas_call(
        lambda *refs: group_faces_kernel(classes, blocks, group, *refs),
        out_shape=(
            jax.ShapeDtypeStruct((rows, LANES), f32),
            *[jax.ShapeDtypeStruct((n, group_size), f32) for n in group_rows],
        ),
        in_specs=[VMEM] * (len(prepared) + 2 + len(held)),
        out_specs=(VMEM,) * (bits + 2),
        scratch_shapes=[
            pltpu.VMEM(kept, f32),
            pltpu.VMEM(kept, f32),
            pltpu.VMEM((8 * tiles + 32, LANES), f32),
            pltpu.VMEM((2 * len(classes), LANES), f32),
            pltpu.VMEM((2 * len(classes), LANES), f32),
        ],
        cost_estimate=pl.CostEstimate(flops=COST[1], bytes_accessed=1 << 20, transcendentals=0),
        compiler_params=pltpu.CompilerParams(vmem_limit_bytes=6 * 2**20),
        name="group_faces",
    )(*prepared, *patch_terms, *held)


def scatter_kernel(rows, bits, own_ref, sub_ref, pat_ref, direct_ref, outer_ref, inner_ref, *refs):
    out_ref = refs[-1]
    row_iota = iota((rows, LANES), 0)
    lane_iota = iota((LANES, LANES), 0)
    odd = jnp.broadcast_to(lax.axis_index("patch") & 1, (1, LANES)) == 1
    direct = direct_ref[0:1, :]
    below, above = by_side((lax.axis_index("patch") >> 1) & 1, outer_ref, inner_ref)
    group_back = refs[0][...]
    for i in range(bits):
        ref = refs[i + 1]
        for at in range(0, ref.shape[0], 1 << (bits - 1 - i)):
            group_back = group_back + ref[at : at + 1, :]
    backs = [
        group_back,
        jnp.where(odd, direct_ref[1:2, :], direct),
        above[0:1],
        jnp.where(odd, direct, direct_ref[1:2, :]),
        below[0:1],
    ]
    left, right = [], []
    for j in range(5):
        index = sub_ref[0:1, :] if j == 0 else pat_ref[j - 1 : j, :]
        value = backs[j]
        width = index.shape[1]
        hi = value.astype(jnp.bfloat16).astype(jnp.float32)
        match = jnp.broadcast_to(index >> 7, (rows, width)) == row_iota[:, :width]
        a_hi = jnp.where(match, jnp.broadcast_to(hi, (rows, width)), 0.0)
        a_lo = jnp.where(match, jnp.broadcast_to(value - hi, (rows, width)), 0.0)
        left.append(jnp.concatenate([a_hi, a_lo], axis=0).astype(jnp.bfloat16))
        spot = jnp.broadcast_to(index & (LANES - 1), (LANES, width)) == lane_iota[:, :width]
        right.append(jnp.where(spot, 1.0, 0.0).astype(jnp.bfloat16))
    product = 0.0
    for part in ([0], [1, 2, 3, 4]) if left[0].shape[1] < LANES else ([0, 1, 2, 3, 4],):
        product = product + lax.dot_general(
            jnp.concatenate([left[j] for j in part], axis=1),
            jnp.concatenate([right[j] for j in part], axis=1),
            (((1,), (1,)), ((), ())),
            preferred_element_type=jnp.float32,
        )
    out_ref[...] = own_ref[...] + product[:rows] + product[rows:]


def in_hbm(*arrays):
    return [pltpu.with_memory_space_constraint(array, pltpu.HBM) for array in arrays]


def stack(parts):
    return parts[0] if len(parts) == 1 else jnp.concatenate(parts, axis=0)


def per_device(heat, basis, area, corners, send_sub, send_pat, live_faces):
    owned = heat.shape[0]
    rows = owned // LANES
    group = lax.axis_size("sub")
    group_size = send_sub.shape[0]
    block_size = send_pat.shape[1]
    offsets = send_pat.shape[0]
    remote_len = group * group_size + offsets * block_size
    blocks = remote_len // (2 * LANES)
    assert offsets == 4 and block_size == LANES and LANES % group_size == 0
    assert group & (group - 1) == 0 and group * group_size % (2 * LANES) == 0
    assert lax.axis_size("patch") % 4 == 0 and corners.shape[1] % (8 * blocks * LANES) == 0
    bits = group.bit_length() - 1
    f32 = jnp.float32
    heat2 = heat.reshape(rows, LANES)
    sub2 = send_sub.reshape(1, group_size)

    mine, near, outer, inner, sub_index, pat_index = pl.pallas_call(
        lambda *refs: send_kernel(rows, *refs),
        out_shape=(
            jax.ShapeDtypeStruct((1, group_size), f32),
            jax.ShapeDtypeStruct((1, LANES), f32),
            jax.ShapeDtypeStruct((2, LANES), f32),
            jax.ShapeDtypeStruct((2, LANES), f32),
            jax.ShapeDtypeStruct(sub2.shape, jnp.int32),
            jax.ShapeDtypeStruct(send_pat.shape, jnp.int32),
        ),
        in_specs=[HBM] * 3,
        out_specs=(VMEM,) * 6,
        scratch_shapes=[
            pltpu.VMEM(heat2.shape, f32),
            pltpu.SemaphoreType.DMA((3,)),
        ],
        compiler_params=pltpu.CompilerParams(vmem_limit_bytes=2 * 2**20),
        name="send_gather",
    )(*in_hbm(heat2, sub2, send_pat))
    prepared = prepare_call(live_faces, heat2, corners, basis, area, blocks)
    place = lax.axis_index("patch")
    take_inner = ((place >> 1) & 1) == (place & 1)
    outer = shift(outer, "patch", 2)
    inner = shift(inner, "patch", -2)
    relay = jnp.where((place & 1) == 0, inner[1:2], outer[1:2])
    direct = swap(jnp.concatenate([near, relay]), "patch", 1)
    held = [mine]
    for bit in range(bits):
        held.append(swap(stack(held), "sub", mask_of(bit)))

    *patch_terms, near, outer, inner = patch_faces_call(prepared, blocks, (direct, outer, inner))
    own_sums, keep, *outs = group_faces_call(prepared, blocks, patch_terms, rows, group, group_size, held)

    outer = swap_far(outer, "patch", True)
    inner = swap_far(inner, "patch", False)
    relay = jnp.where(take_inner, inner[1:2], outer[1:2])
    direct = swap(jnp.concatenate([near, relay]), "patch", 1)
    pieces, group_back = [], []
    for bit in reversed(range(bits)):
        width = 1 << bit
        got = swap(stack([outs[bit]] + [p[width : 2 * width] for p in pieces]), "sub", mask_of(bit))
        group_back.append(got)
        pieces = [p[:width] for p in pieces] + [
            got[at : at + width] for at in range(0, got.shape[0], width)
        ]

    result = pl.pallas_call(
        lambda *refs: scatter_kernel(rows, bits, *refs),
        out_shape=jax.ShapeDtypeStruct((rows, LANES), f32),
        in_specs=[VMEM] * (7 + bits),
        out_specs=VMEM,
        compiler_params=pltpu.CompilerParams(vmem_limit_bytes=4 * 2**20),
        name="scatter_back",
    )(own_sums, sub_index, pat_index, direct, outer, inner, keep, *group_back)
    return result.reshape(-1)


def solution(mesh):
    placed = (
        P(("patch", "sub")),
        P(None, ("patch", "sub")),
        P(("patch", "sub")),
        P(None, ("patch", "sub")),
        P(("patch", "sub")),
        P(None, ("patch", "sub")),
        P(("patch", "sub")),
    )

    return jax.shard_map(per_device, mesh=mesh, in_specs=placed, out_specs=P(("patch", "sub")), check_vma=False)
```
